32 devices in a mesh: rep: 8 (over y, x, core), tp: 4 (over z).
Axes of the slice: x: 2, y: 2, z: 4, core: 2. Of those that a mesh axis runs over, the one named last changes fastest.
Arguments:
- hidden: bfloat16 [512, 8192], P('rep'), may hold values from -6 to 6
- norm_gain: bfloat16 [8192], replicated, may hold values from 0.5 to 1.5
- query_weight_matrix: bfloat16 [8192, 4096], P(None, 'tp'), may hold values from -0.0625 to 0.0625
- key_value_weight: bfloat16 [2, 8192, 1024], P(None, None, 'tp'), may hold values from -0.0625 to 0.0625
- output_weight_matrix: bfloat16 [4096, 8192], P('tp'), may hold values from -0.375 to 0.375
- input_down_factors: bfloat16 [3, 8192, 64], P(None, ('rep', 'tp')), may hold values from -0.0625 to 0.0625
- query_up_factor: bfloat16 [64, 4096], P(None, ('rep', 'tp')), may hold values from -0.75 to 0.75
- key_value_up_factors: bfloat16 [2, 64, 1024], P(None, None, ('rep', 'tp')), may hold values from -0.75 to 0.75
- output_down_factor: bfloat16 [4096, 64], P(('rep', 'tp')), may hold values from -0.375 to 0.375
- output_up_factor: bfloat16 [64, 8192], P(None, ('rep', 'tp')), may hold values from -0.75 to 0.75
- cache_keys: bfloat16 [512, 8, 128, 128], P('rep', 'tp'), may hold values from -360 to 360
- cache_values: bfloat16 [512, 8, 128, 128], P('rep', 'tp'), may hold values from -6 to 6
- lengths: int32 [512], P('rep'), may hold values from 1 to 127
Outputs:
- attn_out: bfloat16 [512, 8192], P('rep', 'tp')
The draws below stay inside these ranges and needn't reach their ends.
All inputs are finite; a program needn't handle non-finite values.
Results may differ from the reference program's by a relative error of at most 0.03.
Values may be sent and summed in bfloat16 or wider, within the bound.
A program may use at most 128 MiB of HBM per device.

```python
import math
import jax
import jax.numpy as jnp
from jax import lax

D = 8192
HEADS = 32
KV_HEADS = 8
HEAD_DIM = 128
RANK = 64
CACHE = 128
BATCH = 512


def draw_cache_keys(key, part):
    base_key = jax.random.fold_in(key, 11)
    values = jax.random.normal(base_key, (BATCH, KV_HEADS, CACHE, HEAD_DIM), jnp.float32)
    values = jnp.clip(values, -6.0, 6.0)
    return values.astype(jnp.bfloat16)


def set_ends(array, key, least, largest):
    spot = [jax.random.randint(jax.random.fold_in(key, axis), (), 0, length) for axis, length in enumerate(array.shape)]
    widest = array.shape.index(max(array.shape))
    next_to = spot[:widest] + [(spot[widest] + 1) % array.shape[widest]] + spot[widest + 1:]
    return array.at[tuple(spot)].set(least).at[tuple(next_to)].set(largest)


def levels(stream_key, dims, shards, least, largest):
    factor_of, own = 1.0, jax.random.fold_in(stream_key, 6)
    for axis_at, blocks in shards:
        heights = jnp.exp(jax.random.uniform(jax.random.fold_in(own, axis_at), (blocks,), jnp.float32, least / len(shards), largest / len(shards)))
        factor_of = factor_of * jnp.repeat(heights, dims[axis_at] // blocks).reshape([-1 if axis == axis_at else 1 for axis in range(len(dims))])
    return factor_of


def normal_values(rng, extent, scale, most, pieces=(), held_as=jnp.bfloat16):
    entries = jax.random.normal(rng, extent, jnp.float32) * scale
    if len(pieces) > 0:
        entries = levels(rng, extent, pieces, -0.22, 0.18) * entries
    return jnp.clip(entries, min=-most, max=most).astype(held_as)


def setup_inputs(seed: int = 0) -> dict:
    key_list = jax.random.split(jax.random.key(seed), 14)
    hidden = normal_values(key_list[0], (BATCH, D), 1.0, 6.0, ((0, 8),))
    norm_gain = jnp.clip(1.0 + 0.1 * jax.random.normal(key_list[1], (D,), jnp.float32), 0.5, 1.5).astype(jnp.bfloat16)
    query_weight_matrix = normal_values(key_list[2], (D, HEADS * HEAD_DIM), D ** -0.5, 0.0625, ((1, 4),))
    key_value_weight = normal_values(key_list[3], (2, D, KV_HEADS * HEAD_DIM), D ** -0.5, 0.0625, ((2, 4),))
    output_weight_matrix = normal_values(key_list[4], (HEADS * HEAD_DIM, D), (HEADS * HEAD_DIM // 16) ** -0.5, 0.375, ((0, 4),))
    input_down_factors = normal_values(key_list[5], (3, D, RANK), D ** -0.5, 0.0625, ((1, 32),))
    query_up_factor = normal_values(key_list[6], (RANK, HEADS * HEAD_DIM), RANK ** -0.5, 0.75, ((1, 32),))
    key_value_up_factors = normal_values(key_list[7], (2, RANK, KV_HEADS * HEAD_DIM), RANK ** -0.5, 0.75, ((2, 32),))
    output_down_factor = normal_values(key_list[8], (HEADS * HEAD_DIM, RANK), (HEADS * HEAD_DIM // 16) ** -0.5, 0.375, ((0, 32),))
    output_up_factor = normal_values(key_list[9], (RANK, D), RANK ** -0.5, 0.75, ((1, 32),))
    cache_keys = draw_cache_keys(jax.random.fold_in(key_list[13], 71), 0)
    cache_values = normal_values(key_list[11], (BATCH, KV_HEADS, CACHE, HEAD_DIM), 1.0, 6.0, ((0, 8), (1, 4)))
    lengths = set_ends(jax.random.randint(key_list[12], (BATCH,), 1, CACHE), jax.random.fold_in(key_list[12], 1), 1, CACHE - 1).astype(jnp.int32)
    return dict(hidden=hidden, norm_gain=norm_gain, query_weight_matrix=query_weight_matrix, key_value_weight=key_value_weight, output_weight_matrix=output_weight_matrix, input_down_factors=input_down_factors, query_up_factor=query_up_factor, key_value_up_factors=key_value_up_factors, output_down_factor=output_down_factor, output_up_factor=output_up_factor, cache_keys=cache_keys, cache_values=cache_values, lengths=lengths)


epsilon = 1e-06
rope_base = 1000000.0
adapter_scale = 0.5

def rope_angles(lengths, head_dim):
    half_dim = head_dim // 2
    frequency = rope_base ** (-(jnp.arange(half_dim, dtype=jnp.float32) * 2.0) / head_dim)
    return lengths.astype(jnp.float32)[:, None] * frequency[None, :]

def rotate(vectors, angles):
    half_dim = vectors.shape[-1] // 2
    cosine = jnp.cos(angles)[:, None, :]
    sine_part = jnp.sin(angles)[:, None, :]
    low_half = vectors[..., :half_dim]
    high_half = vectors[..., half_dim:]
    return jnp.concatenate([low_half * cosine - high_half * sine_part, high_half * cosine + low_half * sine_part], axis=-1)

def adapted(normed, frozen_matrix, inner_part, up_factor):
    base_part = jnp.dot(normed, frozen_matrix, preferred_element_type=jnp.float32)
    return base_part + adapter_scale * jnp.dot(inner_part, up_factor, preferred_element_type=jnp.float32)

def attend(query, new_key, new_value, keys, values, lengths):
    score_scale = 1.0 / math.sqrt(keys.shape[-1])
    scores = jnp.einsum('bkgd,bkld->bkgl', query, keys.astype(jnp.float32), precision=lax.Precision.HIGHEST) * score_scale
    own_score = lax.optimization_barrier(jnp.sum(query * new_key.astype(jnp.float32)[:, :, None, :], axis=-1)) * score_scale
    live_mask = jnp.arange(keys.shape[2], dtype=jnp.int32)[None, None, None, :] < lengths[:, None, None, None]
    row_max = jnp.maximum(lax.optimization_barrier(jnp.max(jnp.where(live_mask, scores, -1e+30), axis=-1)), own_score)
    weights = jnp.where(live_mask, jnp.exp(scores - row_max[..., None]), 0.0)
    own_weight = jnp.exp(own_score - row_max)
    denom_sum = lax.optimization_barrier(jnp.sum(weights, axis=-1)) + own_weight
    probs = (weights / denom_sum[..., None]).astype(jnp.bfloat16)
    own_prob = (own_weight / denom_sum).astype(jnp.bfloat16)
    context = jnp.einsum('bkgl,bkld->bkgd', probs.astype(jnp.float32), values.astype(jnp.float32))
    context = context + own_prob.astype(jnp.float32)[..., None] * new_value.astype(jnp.float32)[:, :, None, :]
    return context.astype(jnp.bfloat16)

def reference(hidden, norm_gain, query_weight_matrix, key_value_weight, output_weight_matrix, input_down_factors, query_up_factor, key_value_up_factors, output_down_factor, output_up_factor, cache_keys, cache_values, lengths):
    states = hidden.astype(jnp.float32)
    square = lax.optimization_barrier(jnp.mean(states * states, axis=-1, keepdims=True))
    normed = (states * lax.rsqrt(square + epsilon) * norm_gain.astype(jnp.float32)).astype(jnp.bfloat16)
    inner_query = jnp.dot(normed, input_down_factors[0], preferred_element_type=jnp.float32).astype(jnp.bfloat16)
    inner_key = jnp.dot(normed, input_down_factors[1], preferred_element_type=jnp.float32).astype(jnp.bfloat16)
    inner_value = jnp.dot(normed, input_down_factors[2], preferred_element_type=jnp.float32).astype(jnp.bfloat16)
    batch = hidden.shape[0]
    kv_count = cache_keys.shape[1]
    head_dim = cache_keys.shape[3]
    angles = rope_angles(lengths, head_dim)
    query = adapted(normed, query_weight_matrix, inner_query, query_up_factor).reshape(batch, -1, head_dim)
    query = rotate(query, angles).reshape(batch, kv_count, -1, head_dim)
    new_key = adapted(normed, key_value_weight[0], inner_key, key_value_up_factors[0]).reshape(batch, kv_count, head_dim)
    new_key = rotate(new_key, angles).astype(jnp.bfloat16)
    new_value = adapted(normed, key_value_weight[1], inner_value, key_value_up_factors[1]).reshape(batch, kv_count, head_dim).astype(jnp.bfloat16)
    context = attend(query, new_key, new_value, cache_keys, cache_values, lengths).reshape(batch, -1)
    middle = jnp.dot(context, output_down_factor, preferred_element_type=jnp.float32).astype(jnp.bfloat16)
    return adapted(context, output_weight_matrix, middle, output_up_factor).astype(jnp.bfloat16)
```

```python
import functools
import math

import jax
import jax.numpy as jnp
from jax import lax
from jax.experimental import pallas as pl
from jax.experimental.pallas import tpu as pltpu
from jax.sharding import PartitionSpec as P

epsilon = 1e-06
rope_base = 1000000.0
adapter_scale = 0.5

f32 = jnp.float32
bf16 = jnp.bfloat16
LANES = 128
MESH_ID = pl.DeviceIdType.MESH


def nt_dot(left, right):
    return lax.dot_general(
        left, right, (((1,), (1,)), ((), ())), preferred_element_type=f32
    )


def nn_dot(left, right):
    return jnp.dot(left, right, preferred_element_type=f32)


def kernel(
    dims,
    hidden,
    gain,
    wq,
    wkv,
    wo,
    dn_own,
    f_q,
    f_kv,
    f_od,
    f_ou,
    cache_k,
    cache_v,
    lengths,
    out,
    gain_b,
    len_b,
    hid_b,
    norm_b,
    wq_b,
    wkv_b,
    wo_b,
    k_b,
    v_b,
    dn_b,
    a_q,
    a_kv,
    a_od,
    a_ou,
    g_q,
    g_kv,
    g_od,
    g_ou,
    angle,
    q_acc,
    kv_acc,
    inner_s,
    inner_r,
    q3,
    nk3,
    nv3,
    c3,
    top3,
    sum3,
    ctx,
    mid_s,
    mid_r,
    part_f,
    own_acc,
    rs_s,
    rs_r,
    small_sem,
    hid_sem,
    w_sem,
    kv_sem,
    wo_sem,
    k_sem,
    v_sem,
    own_sem,
    dn_ssem,
    dn_rsem,
    dn_fsem,
    a_ssem,
    a_rsem,
    g_ssem,
    g_rsem,
    g_fsem,
    in_ssem,
    in_rsem,
    mid_ssem,
    mid_rsem,
    rs_ssem,
    rs_rsem,
):
    n, reps = dims["tp"], dims["rep"]
    seqs, depth = hidden.shape
    head_dim = cache_k.shape[3]
    kv_local = cache_k.shape[1]
    heads = wq.shape[1] // head_dim
    group = heads // kv_local
    pad_heads = q3.shape[0] // seqs
    rank = dims["rank"]
    block, win = dims["block"], dims["win"]
    half_reps = reps // 2
    r = lax.axis_index("rep")
    t = lax.axis_index("tp")
    core = lax.rem(r, 2)
    partner = r + 1 - 2 * core

    barrier = pltpu.get_barrier_semaphore()

    def greet(rr, tt):
        pl.semaphore_signal(barrier, inc=1, device_id=(rr, tt), device_id_type=MESH_ID)

    count = 0
    for j in range(n - 1, 0, -1):
        greet(r, lax.rem(t + j, n))
        count += 1
    for j in range(1, half_reps):
        greet(lax.rem(r + 2 * j, reps), t)
        count += 1
    greet(partner, t)
    count += 1

    hid = pltpu.make_async_copy(hidden, hid_b, hid_sem)
    hid.start()
    gain_in = pltpu.make_async_copy(gain, gain_b, small_sem.at[0])
    gain_in.start()
    len_in = pltpu.make_async_copy(lengths, len_b, small_sem.at[1])
    len_in.start()
    own_dn = pltpu.make_async_copy(dn_own, dn_b.at[r], own_sem.at[0])
    mine_at = r // 2
    spread = (a_q, a_kv, a_od, a_ou)
    gathered = (g_q, g_kv, g_od, g_ou)
    own_f = [
        pltpu.make_async_copy(src, dst.at[mine_at], own_sem.at[1 + f])
        for f, (src, dst) in enumerate(zip((f_q, f_kv, f_od, f_ou), spread))
    ]
    own_dn.start()
    for c in own_f:
        c.start()
    steps = w_sem.shape[0]
    kc = depth // steps

    def w_copies(i):
        rows = pl.ds(pl.multiple_of(i * kc, kc), kc)
        return (
            pltpu.make_async_copy(wq.at[rows, :], wq_b.at[rows, :], w_sem.at[i]),
            pltpu.make_async_copy(wkv.at[:, rows, :], wkv_b.at[:, rows, :], kv_sem.at[i]),
        )

    @pl.loop(0, steps)
    def _(i):
        for c in w_copies(i):
            c.start()

    parts = k_sem.shape[0]
    ps = seqs // parts

    def cache_copies(i):
        rows = pl.ds(i * ps, ps)
        return (
            pltpu.make_async_copy(cache_k.at[rows], k_b.at[rows], k_sem.at[i]),
            pltpu.make_async_copy(cache_v.at[rows], v_b.at[rows], v_sem.at[i]),
        )

    wide = wo.shape[1] // n
    most, least = jnp.maximum(n - 1 - t, t), jnp.minimum(n - 1 - t, t)
    toward = jnp.where(n - 1 - t > t, 1, -1)

    def dest(i):
        lead = most - least
        late = jnp.maximum(i - lead, 0)
        away = least - late // 2
        side = jnp.where(late % 2 == 0, -toward, toward)
        return t + jnp.where(i < lead, toward * (most - i), side * away)

    def wo_copy(d):
        cols = pl.ds(pl.multiple_of(d * wide, LANES), wide)
        return pltpu.make_async_copy(wo.at[:, cols], wo_b.at[d], wo_sem.at[d])

    @pl.loop(0, parts)
    def _(i):
        for c in cache_copies(i):
            c.start()

    @pl.loop(0, n - 1)
    def _(i):
        wo_copy(dest(i)).start()

    wo_copy(t).start()

    def remote(src, dst, ssem, rsem, rr, tt):
        return pltpu.make_async_remote_copy(
            src_ref=src,
            dst_ref=dst,
            send_sem=ssem,
            recv_sem=rsem,
            device_id=(rr, tt),
            device_id_type=MESH_ID,
        )

    pl.semaphore_wait(barrier, count)
    ranks = (pl.ds(0, rank), pl.ds(rank, 2 * rank))
    dn_sends = []

    def down(src, part, ssem, rr):
        here = dn_b.at[src, ranks[part]]
        return remote(here, here, ssem, dn_rsem.at[part, src], rr, t)

    def send_down(part):
        for j in range(1, half_reps):
            dn_sends.append(down(r, part, dn_ssem.at[part, j], lax.rem(r + 2 * j, reps)))
        dn_sends.append(down(r, part, dn_fsem.at[part, 0], partner))
        for c in dn_sends[-half_reps:]:
            c.start()

    def relay_down(part):
        for j in range(half_reps - 1, 0, -1):
            src = lax.rem(r + 2 * j, reps)
            c = down(src, part, dn_fsem.at[part, j], partner)
            c.wait_recv()
            c.start()
            dn_sends.append(c)

    def share_inner(part):
        for j in range(half_reps):
            src = lax.rem(partner + 2 * j, reps)
            down(src, part, dn_fsem.at[part, j], partner).wait_recv()
        total = jnp.zeros((seqs, (1 + part) * rank), f32)
        for j in range(reps):
            start = (j * n + t) * block
            cols = pl.ds(pl.multiple_of(start // win * win, LANES), win)
            total = total + nt_dot(norm_b[:, cols], dn_b[j, ranks[part]])
        sends = share(
            packed(total), inner_s.at[part], inner_r.at[part], in_ssem.at[part], in_rsem.at[part]
        )
        return sends, total

    fold = max(1, LANES // rank)
    few = seqs // fold

    def packed(x):
        if x.shape[1] != rank:
            return x
        return jnp.concatenate([x[f * few : (f + 1) * few] for f in range(fold)], axis=1)

    def unpacked(x):
        return jnp.concatenate([x[:, f * rank : (f + 1) * rank] for f in range(fold)], axis=0)

    def share(x, own, others, ssem, rsem):
        size = x.shape[0]
        own[pl.ds(0, size), :] = x.astype(bf16)
        made = []
        for j in range(1, n):
            c = remote(
                own.at[pl.ds(0, size)], others.at[j, pl.ds(0, size)], ssem.at[j], rsem.at[j],
                r, lax.rem(t + j, n),
            )
            c.start()
            made.append(c)
        return made

    def gather_sum(total, sends, others):
        for c in sends:
            c.wait_recv()
        for j in range(1, n):
            got = others[j] if total.shape[1] != rank else unpacked(others[j, :few])
            total = total + got.astype(f32)
        return total.astype(bf16)

    a_sends = []

    def to_chips(f):
        buf = spread[f]
        own_f[f].wait()
        for j in range(1, half_reps):
            c = remote(
                buf.at[mine_at], buf.at[mine_at], a_ssem.at[f, j], a_rsem.at[f, mine_at],
                lax.rem(r + 2 * j, reps), t,
            )
            c.start()
            a_sends.append(c)

    per_plane = reps // n
    groups = per_plane // 2
    g_sends = []

    def to_planes(f):
        buf, full = spread[f], gathered[f]
        for j in range(1, half_reps):
            src = lax.rem(r + 2 * j, reps) // 2
            remote(
                buf.at[src], buf.at[src], a_ssem.at[f, j], a_rsem.at[f, src], r, t
            ).wait_recv()
        for i in range(groups):
            s = n * (2 * i + core) + t
            for j in range(1, n):
                plane = lax.rem(t + j, n)
                src = (plane * per_plane + 2 * i) // 2
                c = remote(
                    buf.at[src], full.at[s], g_ssem.at[f, i * n + j], g_rsem.at[f, s],
                    r, plane,
                )
                c.start()
                g_sends.append(c)
            src = (t * per_plane + 2 * i) // 2
            pltpu.make_async_copy(buf.at[src], full.at[s], g_rsem.at[f, s]).start()

    def across(f):
        full = gathered[f]
        for i in range(groups):
            for z in range(n):
                s = n * (2 * i + core) + z
                pltpu.make_async_copy(spread[f].at[0], full.at[s], g_rsem.at[f, s]).wait()
                c = remote(
                    full.at[s], full.at[s], g_fsem.at[f, i * n + z], g_rsem.at[f, s],
                    partner, t,
                )
                c.start()
                g_sends.append(c)

    def settled(f):
        full = gathered[f]
        for i in range(groups):
            for z in range(n):
                s = n * (2 * i + 1 - core) + z
                pltpu.make_async_copy(spread[f].at[0], full.at[s], g_rsem.at[f, s]).wait()

    to_chips(0)
    own_dn.wait()
    send_down(0)
    to_chips(1)
    send_down(1)
    to_chips(2)
    to_chips(3)

    gain_in.wait()
    hid.wait()

    @pl.loop(0, seqs // 16)
    def _(i):
        rows = pl.ds(pl.multiple_of(i * 16, 16), 16)
        x = hid_b[rows, :].astype(f32)
        square = jnp.mean(x * x, axis=-1, keepdims=True)
        norm_b[rows, :] = (
            x * lax.rsqrt(square + epsilon) * gain_b[...].astype(f32).reshape(1, depth)
        ).astype(bf16)

    q_acc[...] = jnp.zeros_like(q_acc)
    kv_acc[...] = jnp.zeros_like(kv_acc)
    both = 2 * kc

    def project(lo, hi):
        @pl.loop(lo, hi)
        def _(i):
            for j in range(2):
                for c in w_copies(2 * i + j):
                    c.wait()
            rows = pl.ds(pl.multiple_of(i * both, both), both)
            x = norm_b[:, rows]
            q_acc[...] += nn_dot(x, wq_b[rows, :])
            for j in range(2):
                kv_acc[j] += nn_dot(x, wkv_b[j, rows, :])

    project(0, 3)
    to_planes(0)
    project(3, 5)
    relay_down(0)
    project(5, 6)
    to_planes(1)
    q_sends, q_part = share_inner(0)
    project(6, 8)
    len_in.wait()

    half_dim = head_dim // 2
    step = lax.rem(lax.broadcasted_iota(jnp.int32, (1, head_dim), 1), half_dim)
    frequency = jnp.exp(step.astype(f32) * (-2.0 * math.log(rope_base) / head_dim))

    @pl.loop(0, seqs // 8)
    def _(i):
        for b in range(8):
            angle[pl.ds(i * 8 + b, 1), :] = len_b[i * 8 + b].astype(f32) * frequency

    cosv = jnp.cos(angle[...])
    sinv = jnp.sin(angle[...])
    lane = lax.broadcasted_iota(jnp.int32, (seqs, head_dim), 1)
    sinv = jnp.where(lane < half_dim, -sinv, sinv)

    def turn(x):
        return x * cosv + pltpu.roll(x, head_dim // 2, 1) * sinv

    across(0)
    relay_down(1)
    across(1)
    kv_sends, kv_part = share_inner(1)
    settled(0)
    inner_q = gather_sum(q_part, q_sends, inner_r.at[0])
    q_up = jnp.concatenate([g_q[s] for s in range(reps)], axis=1)
    q = q_acc[...] + adapter_scale * nn_dot(inner_q, q_up)
    for h in range(pad_heads):
        rows = pl.ds(h, seqs, stride=pad_heads)
        if h < heads:
            q3[rows, :] = turn(q[:, h * head_dim : (h + 1) * head_dim])
        else:
            q3[rows, :] = jnp.zeros((seqs, head_dim), f32)

    def rows_of(j):
        w = g_kv.shape[2]
        return g_kv[:, j].astype(f32).reshape(reps * w, rank).astype(bf16)

    def new_pair():
        inner = gather_sum(kv_part, kv_sends, inner_r.at[1]).astype(f32)
        inner_k = inner[:, :rank].astype(bf16)
        inner_v = inner[:, rank:].astype(bf16)
        nk = kv_acc[0] + adapter_scale * nt_dot(inner_k, rows_of(0))
        nv = kv_acc[1] + adapter_scale * nt_dot(inner_v, rows_of(1))
        for j in range(kv_local):
            key = turn(nk[:, j * head_dim : (j + 1) * head_dim]).astype(bf16).astype(f32)
            val = nv[:, j * head_dim : (j + 1) * head_dim].astype(bf16).astype(f32)
            for g in range(pad_heads):
                if min(g // group, kv_local - 1) == j:
                    rows = pl.ds(g, seqs, stride=pad_heads)
                    nk3[rows, :] = key
                    nv3[rows, :] = val

    cache = cache_k.shape[2]
    span = kv_local * cache
    score_scale = 1.0 / math.sqrt(head_dim)
    bs = min(16, ps)
    per = ps // bs

    def attend(i):
        @pl.when(lax.rem(i, per) == 0)
        def _():
            for c in cache_copies(i // per):
                c.wait()

        base = pl.multiple_of(i * (bs * pad_heads), bs * pad_heads)
        rows = pl.ds(base, bs * pad_heads)
        qq = q3[rows, :]
        hi = qq.astype(bf16).astype(f32)
        rest = qq - hi
        mid = rest.astype(bf16).astype(f32)
        low = rest - mid
        row_id = lax.broadcasted_iota(jnp.int32, (pad_heads, span), 0)
        col_id = lax.broadcasted_iota(jnp.int32, (pad_heads, span), 1)
        mine = jnp.minimum(row_id // group, kv_local - 1) == col_id // cache
        pos = lax.rem(col_id, cache)
        scored = []
        for b in range(bs):
            sl = slice(b * pad_heads, (b + 1) * pad_heads)
            stack = jnp.concatenate([hi[sl], mid[sl], low[sl]], axis=0).astype(bf16)
            keys = k_b[i * bs + b].reshape(span, head_dim)
            dots = nt_dot(stack, keys)
            sc = (
                dots[:pad_heads]
                + dots[pad_heads : 2 * pad_heads]
                + dots[2 * pad_heads :]
            ) * score_scale
            live = jnp.logical_and(mine, pos < len_b[i * bs + b])
            scored.append(jnp.where(live, sc, -1e30))
        sc = jnp.concatenate(scored, axis=0)
        top = jnp.max(sc, axis=-1, keepdims=True)
        w = jnp.exp(sc - top)
        top3[rows, :] = jnp.broadcast_to(top, (bs * pad_heads, head_dim))
        sum3[rows, :] = jnp.broadcast_to(
            jnp.sum(w, axis=-1, keepdims=True), (bs * pad_heads, head_dim)
        )
        for b in range(bs):
            sl = slice(b * pad_heads, (b + 1) * pad_heads)
            vals = v_b[i * bs + b].reshape(span, head_dim)
            here = pl.ds(base + b * pad_heads, pad_heads)
            c3[here, :] = nn_dot(w[sl].astype(bf16), vals)

    def merge(i):
        rows = pl.ds(i * (bs * pad_heads), bs * pad_heads)
        own = jnp.sum(q3[rows, :] * nk3[rows, :], axis=-1, keepdims=True) * score_scale
        top = jnp.maximum(top3[rows, :], own)
        old = jnp.exp(top3[rows, :] - top)
        new = jnp.exp(own - top)
        scale = 1.0 / (sum3[rows, :] * old + new)
        c3[rows, :] = c3[rows, :] * (old * scale) + (new * scale).astype(bf16).astype(
            f32
        ) * nv3[rows, :]

    waves = rs_ssem.shape[1]
    ws = seqs // waves
    tile = min(1024, wide)

    def finish_wave(wave):
        for i in range(wave * ws // bs, (wave + 1) * ws // bs):
            merge(i)
        for h in range(heads):
            ctx[wave * ws : (wave + 1) * ws, h * head_dim : (h + 1) * head_dim] = c3[
                pl.ds(wave * ws * pad_heads + h, ws, stride=pad_heads), :
            ].astype(bf16)

    def hop(d, wave, up):
        rows = pl.ds(pl.multiple_of(wave * ws, ws), ws)
        slot = d + up
        return remote(
            rs_s.at[d, rows], rs_r.at[slot, rows], rs_ssem.at[d, wave],
            rs_rsem.at[slot, wave], r, t + 2 * up - 1,
        )

    def pass_on(i, wave):
        d = dest(i)
        up = jnp.where(d > t, 1, 0)
        rows = pl.ds(pl.multiple_of(wave * ws, ws), ws)
        for j in range(wide // tile):
            cols = slice(j * tile, (j + 1) * tile)
            part_f[:, cols] = nn_dot(ctx[rows, :], wo_b[d, :, cols])
        fed = jnp.where(d > t, t > 0, t < n - 1)

        @pl.when(fed)
        def _():
            hop(d, wave, up).wait_recv()
            rs_s[d, rows, :] = (part_f[...] + rs_r[d + up, rows, :].astype(f32)).astype(bf16)

        @pl.when(jnp.logical_not(fed))
        def _():
            rs_s[d, rows, :] = part_f[...].astype(bf16)

        hop(d, wave, up).start()

    pl.loop(0, seqs // bs)(attend)
    to_planes(2)
    to_planes(3)
    settled(1)
    new_pair()
    at_end = jnp.logical_or(t == 0, t == n - 1)
    for wave in range(waves):
        finish_wave(wave)
        if wave == 0:
            wo_copy(dest(0)).wait()

        @pl.when(at_end)
        def _():
            pass_on(0, wave)

    across(2)
    settled(2)
    down_t = jnp.concatenate([g_od[s] for s in range(reps)], axis=1)
    mid_part = nt_dot(ctx[...], down_t)
    mid_sends = share(packed(mid_part), mid_s, mid_r, mid_ssem, mid_rsem)
    across(3)

    @pl.loop(jnp.where(at_end, 1, 0), n - 1)
    def _(i):
        @pl.when(i > 0)
        def _():
            wo_copy(dest(i)).wait()

        @pl.loop(0, waves)
        def _(wave):
            pass_on(i, wave)

    wo_copy(t).wait()
    for j in range(wide // tile):
        cols = slice(j * tile, (j + 1) * tile)
        own_acc[:, cols] = nn_dot(ctx[...], wo_b[t, :, cols])
    settled(3)
    middle = gather_sum(mid_part, mid_sends, mid_r)
    up_full = jnp.concatenate([g_ou[s] for s in range(reps)], axis=1)
    own_acc[...] += adapter_scale * nn_dot(middle, up_full)

    @pl.loop(0, waves)
    def _(wave):
        rows = pl.ds(pl.multiple_of(wave * ws, ws), ws)

        @pl.when(t < n - 1)
        def _():
            hop(t, wave, 0).wait_recv()
            own_acc[rows, :] += rs_r[t, rows, :].astype(f32)

        @pl.when(t > 0)
        def _():
            hop(t, wave, 1).wait_recv()
            own_acc[rows, :] += rs_r[t + 1, rows, :].astype(f32)

        out[rows, :] = own_acc[rows, :].astype(bf16)

    for c in dn_sends + a_sends + g_sends + q_sends + kv_sends + mid_sends:
        c.wait_send()

    @pl.loop(0, n - 1)
    def _(i):
        d = dest(i)

        @pl.loop(0, waves)
        def _(wave):
            hop(d, wave, jnp.where(d > t, 1, 0)).wait_send()


def local(
    hidden,
    norm_gain,
    query_weight_matrix,
    key_value_weight,
    output_weight_matrix,
    input_down_factors,
    query_up_factor,
    key_value_up_factors,
    output_down_factor,
    output_up_factor,
    cache_keys,
    cache_values,
    lengths,
):
    reps, n = lax.axis_size("rep"), lax.axis_size("tp")
    r, t = lax.axis_index("rep"), lax.axis_index("tp")
    seqs, depth = hidden.shape
    _, kv_local, cache, head_dim = cache_keys.shape
    width = query_weight_matrix.shape[1]
    heads = width // head_dim
    rank = input_down_factors.shape[2]
    block = input_down_factors.shape[1]
    win = max(block, LANES)

    down = jnp.swapaxes(input_down_factors, 1, 2).reshape(3 * rank, block)
    if win != block:
        spot = lax.rem((r * n + t) * block, win)
        down = lax.dynamic_update_slice(
            jnp.zeros((3 * rank, win), down.dtype), down, (0, spot)
        )
    f_q = query_up_factor
    f_kv = jnp.swapaxes(key_value_up_factors, 1, 2)
    f_od = output_down_factor.T
    f_ou = output_up_factor
    factors = (f_q, f_kv, f_od, f_ou)
    dims = dict(
        tp=n, rep=reps, rank=rank, block=block, win=win,
    )
    pad_heads = -(-heads // 8) * 8
    wide = depth // n
    rows = seqs * pad_heads
    steps, parts, waves = 16, 4, seqs // 16
    dma = pltpu.SemaphoreType.DMA
    hbm = pl.BlockSpec(memory_space=pl.ANY)
    vmem = pl.BlockSpec(memory_space=pltpu.VMEM)
    vec = pltpu.VMEM
    return pl.pallas_call(
        functools.partial(kernel, dims),
        name="decode_block",
        out_shape=jax.ShapeDtypeStruct((seqs, wide), bf16),
        in_specs=[hbm] * 13,
        out_specs=vmem,
        scratch_shapes=[
            vec((depth,), bf16),
            pltpu.SMEM((seqs,), jnp.int32),
            vec((seqs, depth), bf16),
            vec((seqs, depth), bf16),
            vec((depth, width), bf16),
            vec((2, depth, kv_local * head_dim), bf16),
            vec((n, width, wide), bf16),
            vec((seqs, kv_local, cache, head_dim), bf16),
            vec((seqs, kv_local, cache, head_dim), bf16),
            vec((reps, 3 * rank, win), bf16),
            *[vec((reps // 2,) + f.shape, bf16) for f in factors],
            *[vec((reps,) + f.shape, bf16) for f in factors],
            vec((seqs, head_dim), f32),
            vec((seqs, width), f32),
            vec((2, seqs, kv_local * head_dim), f32),
            vec((2, seqs, 2 * rank), bf16),
            vec((2, n, seqs, 2 * rank), bf16),
            *[vec((rows, head_dim), f32)] * 6,
            vec((seqs, width), bf16),
            vec((seqs, 2 * rank), bf16),
            vec((n, seqs, 2 * rank), bf16),
            vec((seqs // waves, wide), f32),
            vec((seqs, wide), f32),
            vec((n, seqs, wide), bf16),
            vec((n + 1, seqs, wide), bf16),
            dma((2,)),
            dma,
            dma((steps,)),
            dma((steps,)),
            dma((n,)),
            dma((parts,)),
            dma((parts,)),
            dma((1 + len(factors),)),
            dma((2, reps // 2)),
            dma((2, reps)),
            dma((2, reps // 2)),
            dma((len(factors), reps // 2)),
            dma((len(factors), reps // 2)),
            dma((len(factors), reps)),
            dma((len(factors), reps)),
            dma((len(factors), reps)),
            dma((2, n)),
            dma((2, n)),
            dma((n,)),
            dma((n,)),
            dma((n, waves)),
            dma((n + 1, waves)),
        ],
        compiler_params=pltpu.CompilerParams(
            collective_id=0, has_side_effects=True, vmem_limit_bytes=66000000
        ),
    )(
        hidden,
        norm_gain,
        query_weight_matrix,
        key_value_weight,
        output_weight_matrix,
        down,
        *factors,
        cache_keys,
        cache_values,
        lengths,
    )


def solution(mesh):
    return jax.shard_map(
        local,
        mesh=mesh,
        in_specs=(
            P("rep", None),
            P(),
            P(None, "tp"),
            P(None, None, "tp"),
            P("tp", None),
            P(None, ("rep", "tp"), None),
            P(None, ("rep", "tp")),
            P(None, None, ("rep", "tp")),
            P(("rep", "tp"), None),
            P(None, ("rep", "tp")),
            P("rep", "tp", None, None),
            P("rep", "tp", None, None),
            P("rep"),
        ),
        out_specs=P("rep", "tp"),
        check_vma=False,
    )
```

```python
import functools
import math

import jax
import jax.numpy as jnp
from jax import lax
from jax.experimental import pallas as pl
from jax.experimental.pallas import tpu as pltpu
from jax.sharding import PartitionSpec as P

epsilon = 1e-06
rope_base = 1000000.0
adapter_scale = 0.5

f32 = jnp.float32
bf16 = jnp.bfloat16
LANES = 128
MESH_ID = pl.DeviceIdType.MESH


def nt_dot(left, right):
    return lax.dot_general(
        left, right, (((1,), (1,)), ((), ())), preferred_element_type=f32
    )


def nn_dot(left, right):
    return jnp.dot(left, right, preferred_element_type=f32)


def kernel(
    dims,
    hidden,
    gain,
    wq,
    wkv,
    wo,
    dn_own,
    f_q,
    f_kv,
    f_od,
    f_ou,
    cache_k,
    cache_v,
    lengths,
    out,
    gain_b,
    len_b,
    hid_b,
    norm_b,
    wq_b,
    wkv_b,
    wo_b,
    k_b,
    v_b,
    dn_b,
    a_q,
    a_kv,
    a_od,
    a_ou,
    g_q,
    g_kv,
    g_od,
    g_ou,
    angle,
    q_acc,
    kv_acc,
    inner_s,
    inner_r,
    q3,
    nk3,
    nv3,
    c3,
    top3,
    sum3,
    ctx,
    mid_s,
    mid_r,
    part_f,
    own_acc,
    rs_s,
    rs_r,
    small_sem,
    hid_sem,
    w_sem,
    kv_sem,
    wo_sem,
    k_sem,
    v_sem,
    own_sem,
    dn_ssem,
    dn_rsem,
    a_ssem,
    a_rsem,
    g_ssem,
    g_rsem,
    g_fsem,
    in_ssem,
    in_rsem,
    mid_ssem,
    mid_rsem,
    rs_ssem,
    rs_rsem,
    ready,
):
    n, reps = dims["tp"], dims["rep"]
    seqs, depth = hidden.shape
    head_dim = cache_k.shape[3]
    kv_local = cache_k.shape[1]
    heads = wq.shape[1] // head_dim
    group = heads // kv_local
    pad_heads = q3.shape[0] // seqs
    rank = dims["rank"]
    block, win = dims["block"], dims["win"]
    half_reps = reps // 2
    r = lax.axis_index("rep")
    t = lax.axis_index("tp")
    core = lax.rem(r, 2)
    partner = r + 1 - 2 * core

    barrier = pltpu.get_barrier_semaphore()

    def greet(rr, tt):
        pl.semaphore_signal(barrier, inc=1, device_id=(rr, tt), device_id_type=MESH_ID)

    count = 0
    below, above = t > 0, t < n - 1

    @pl.when(below)
    def _():
        greet(r, t - 1)

    @pl.when(above)
    def _():
        greet(r, t + 1)

    beside = jnp.where(below, 1, 0) + jnp.where(above, 1, 0)
    for j in range(1, half_reps):
        greet(lax.rem(r + 2 * j, reps), t)
        greet(lax.rem(partner + 2 * j, reps), t)
        count += 2
    greet(partner, t)
    count += 1

    hid = pltpu.make_async_copy(hidden, hid_b, hid_sem)
    hid.start()
    gain_in = pltpu.make_async_copy(gain, gain_b, small_sem.at[0])
    gain_in.start()
    len_in = pltpu.make_async_copy(lengths, len_b, small_sem.at[1])
    len_in.start()
    own_dn = pltpu.make_async_copy(dn_own, dn_b.at[r], own_sem.at[0])
    mine_at = r // 2
    spread = (a_q, a_kv, a_od, a_ou)
    gathered = (g_q, g_kv, g_od, g_ou)
    own_f = [
        pltpu.make_async_copy(src, dst.at[mine_at], own_sem.at[1 + f])
        for f, (src, dst) in enumerate(zip((f_q, f_kv, f_od, f_ou), spread))
    ]
    own_dn.start()
    for c in own_f:
        c.start()
    steps = w_sem.shape[0]
    kc = depth // steps

    def w_copies(i):
        rows = pl.ds(pl.multiple_of(i * kc, kc), kc)
        return (
            pltpu.make_async_copy(wq.at[rows, :], wq_b.at[rows, :], w_sem.at[i]),
            pltpu.make_async_copy(wkv.at[:, rows, :], wkv_b.at[:, rows, :], kv_sem.at[i]),
        )

    @pl.loop(0, steps)
    def _(i):
        for c in w_copies(i):
            c.start()

    parts = k_sem.shape[0]
    ps = seqs // parts

    def cache_copies(i):
        rows = pl.ds(i * ps, ps)
        return (
            pltpu.make_async_copy(cache_k.at[rows], k_b.at[rows], k_sem.at[i]),
            pltpu.make_async_copy(cache_v.at[rows], v_b.at[rows], v_sem.at[i]),
        )

    wide = wo.shape[1] // n
    most, least = jnp.maximum(n - 1 - t, t), jnp.minimum(n - 1 - t, t)
    toward = jnp.where(n - 1 - t > t, 1, -1)

    def dest(i):
        lead = most - least
        late = jnp.maximum(i - lead, 0)
        away = least - late // 2
        side = jnp.where(late % 2 == 0, -toward, toward)
        return t + jnp.where(i < lead, toward * (most - i), side * away)

    def wo_copy(d):
        cols = pl.ds(pl.multiple_of(d * wide, LANES), wide)
        return pltpu.make_async_copy(wo.at[:, cols], wo_b.at[d], wo_sem.at[d])

    @pl.loop(0, parts)
    def _(i):
        for c in cache_copies(i):
            c.start()

    @pl.loop(0, n - 1)
    def _(i):
        wo_copy(dest(i)).start()

    wo_copy(t).start()

    def remote(src, dst, ssem, rsem, rr, tt):
        return pltpu.make_async_remote_copy(
            src_ref=src,
            dst_ref=dst,
            send_sem=ssem,
            recv_sem=rsem,
            device_id=(rr, tt),
            device_id_type=MESH_ID,
        )

    pl.semaphore_wait(barrier, count + beside)

    def tell(k):
        @pl.when(below)
        def _():
            pl.semaphore_signal(
                ready.at[k], inc=1, device_id=(r, t - 1), device_id_type=MESH_ID
            )

        @pl.when(above)
        def _():
            pl.semaphore_signal(
                ready.at[k], inc=1, device_id=(r, t + 1), device_id_type=MESH_ID
            )

    tell(0)
    ranks = (pl.ds(0, rank), pl.ds(rank, 2 * rank))

    def whole(ref, sem):
        return pltpu.make_async_copy(ref, ref, sem)

    def down(src, part, way, rr):
        here = dn_b.at[src, ranks[part]]
        return remote(here, here, dn_ssem.at[part], dn_rsem.at[part, way], rr, t)

    def send_down(part):
        for j in range(1, half_reps):
            down(r, part, 0, lax.rem(partner + 2 * j, reps)).start()
        down(r, part, 1, partner).start()

    def relay_down(part):
        whole(dn_b.at[pl.ds(0, half_reps - 1), ranks[part]], dn_rsem.at[part, 0]).wait()
        for j in range(1, half_reps):
            down(lax.rem(partner + 2 * j, reps), part, 1, partner).start()

    def share_inner(part):
        whole(dn_b.at[pl.ds(0, half_reps), ranks[part]], dn_rsem.at[part, 1]).wait()
        total = jnp.zeros((seqs, (1 + part) * rank), f32)
        for j in range(reps):
            start = (j * n + t) * block
            cols = pl.ds(pl.multiple_of(start // win * win, LANES), win)
            total = total + nt_dot(norm_b[:, cols], dn_b[j, ranks[part]])
        share(packed(total), inner_s.at[part], inner_r.at[part], in_ssem.at[part], in_rsem.at[part])
        return total

    fold = max(1, LANES // rank)
    few = seqs // fold

    def packed(x):
        if x.shape[1] != rank:
            return x
        return jnp.concatenate([x[f * few : (f + 1) * few] for f in range(fold)], axis=1)

    def unpacked(x):
        return jnp.concatenate([x[:, f * rank : (f + 1) * rank] for f in range(fold)], axis=0)

    def share(x, own, others, ssem, rsem):
        size = x.shape[0]
        own[pl.ds(0, size), :] = x.astype(bf16)
        for j in range(1, n):
            remote(
                own.at[pl.ds(0, size)], others.at[j, pl.ds(0, size)], ssem, rsem,
                r, lax.rem(t + j, n),
            ).start()

    def shared(total, others, sem):
        size = few if total.shape[1] == rank else seqs
        return whole(others.at[pl.ds(0, n - 1), pl.ds(0, size)], sem)

    def gather_sum(total, others, rsem):
        shared(total, others, rsem).wait()
        for j in range(1, n):
            got = others[j] if total.shape[1] != rank else unpacked(others[j, :few])
            total = total + got.astype(f32)
        return total.astype(bf16)

    def to_chips(f):
        here = spread[f].at[mine_at]
        own_f[f].wait()
        for j in range(1, half_reps):
            remote(
                here, here, a_ssem.at[f], a_rsem.at[f], lax.rem(r + 2 * j, reps), t
            ).start()

    per_plane = reps // n
    groups = per_plane // 2

    def to_planes(f):
        buf, full = spread[f], gathered[f]
        whole(buf.at[pl.ds(0, half_reps - 1)], a_rsem.at[f]).wait()
        for i in range(groups):
            s = n * (2 * i + core) + t
            for j in range(1, n):
                plane = lax.rem(t + j, n)
                src = (plane * per_plane + 2 * i) // 2
                remote(
                    buf.at[src], full.at[s], g_ssem.at[f], g_rsem.at[f, 0], r, plane
                ).start()
            src = (t * per_plane + 2 * i) // 2
            pltpu.make_async_copy(buf.at[src], full.at[s], g_rsem.at[f, 0]).start()

    def across(f):
        full = gathered[f]
        whole(full.at[pl.ds(0, groups * n)], g_rsem.at[f, 0]).wait()
        for i in range(groups):
            here = full.at[pl.ds(n * (2 * i + core), n)]
            remote(here, here, g_fsem.at[f], g_rsem.at[f, 1], partner, t).start()

    def settled(f):
        whole(gathered[f].at[pl.ds(0, groups * n)], g_rsem.at[f, 1]).wait()

    to_chips(0)
    own_dn.wait()
    send_down(0)
    to_chips(1)
    send_down(1)
    to_chips(2)
    to_chips(3)

    gain_in.wait()
    hid.wait()

    @pl.loop(0, seqs // 16)
    def _(i):
        rows = pl.ds(pl.multiple_of(i * 16, 16), 16)
        x = hid_b[rows, :].astype(f32)
        square = jnp.mean(x * x, axis=-1, keepdims=True)
        norm_b[rows, :] = (
            x * lax.rsqrt(square + epsilon) * gain_b[...].astype(f32).reshape(1, depth)
        ).astype(bf16)

    q_acc[...] = jnp.zeros_like(q_acc)
    kv_acc[...] = jnp.zeros_like(kv_acc)

    def project(i, many):
        for j in range(many):
            for c in w_copies(i + j):
                c.wait()
        rows = pl.ds(pl.multiple_of(i * kc, kc), many * kc)
        x = norm_b[:, rows]
        q_acc[...] += nn_dot(x, wq_b[rows, :])
        for j in range(2):
            kv_acc[j] += nn_dot(x, wkv_b[j, rows, :])

    def heard(k):
        if k < n - 2:
            pl.semaphore_wait(ready.at[k], beside)
        if k < n - 3:
            tell(k + 1)

    project(0, 2)
    heard(0)
    project(2, 2)
    for k in range(1, n - 2):
        heard(k)
    to_planes(0)
    project(4, 1)
    relay_down(0)
    project(5, 1)
    q_part = share_inner(0)
    project(6, 2)
    to_planes(1)
    relay_down(1)
    len_in.wait()

    half_dim = head_dim // 2
    step = lax.rem(lax.broadcasted_iota(jnp.int32, (1, head_dim), 1), half_dim)
    frequency = jnp.exp(step.astype(f32) * (-2.0 * math.log(rope_base) / head_dim))

    @pl.loop(0, seqs // 8)
    def _(i):
        for b in range(8):
            angle[pl.ds(i * 8 + b, 1), :] = len_b[i * 8 + b].astype(f32) * frequency

    cosv = jnp.cos(angle[...])
    sinv = jnp.sin(angle[...])
    lane = lax.broadcasted_iota(jnp.int32, (seqs, head_dim), 1)
    sinv = jnp.where(lane < half_dim, -sinv, sinv)

    def turn(x):
        return x * cosv + pltpu.roll(x, head_dim // 2, 1) * sinv

    across(0)
    kv_part = share_inner(1)
    settled(0)
    inner_q = gather_sum(q_part, inner_r.at[0], in_rsem.at[0])
    q_up = jnp.concatenate([g_q[s] for s in range(reps)], axis=1)
    q = q_acc[...] + adapter_scale * nn_dot(inner_q, q_up)
    for h in range(pad_heads):
        rows = pl.ds(h, seqs, stride=pad_heads)
        if h < heads:
            q3[rows, :] = turn(q[:, h * head_dim : (h + 1) * head_dim])
        else:
            q3[rows, :] = jnp.zeros((seqs, head_dim), f32)

    def rows_of(j):
        w = g_kv.shape[2]
        return g_kv[:, j].astype(f32).reshape(reps * w, rank).astype(bf16)

    def new_pair():
        inner = gather_sum(kv_part, inner_r.at[1], in_rsem.at[1]).astype(f32)
        inner_k = inner[:, :rank].astype(bf16)
        inner_v = inner[:, rank:].astype(bf16)
        nk = kv_acc[0] + adapter_scale * nt_dot(inner_k, rows_of(0))
        nv = kv_acc[1] + adapter_scale * nt_dot(inner_v, rows_of(1))
        for j in range(kv_local):
            key = turn(nk[:, j * head_dim : (j + 1) * head_dim]).astype(bf16).astype(f32)
            val = nv[:, j * head_dim : (j + 1) * head_dim].astype(bf16).astype(f32)
            for g in range(pad_heads):
                if min(g // group, kv_local - 1) == j:
                    rows = pl.ds(g, seqs, stride=pad_heads)
                    nk3[rows, :] = key
                    nv3[rows, :] = val

    cache = cache_k.shape[2]
    span = kv_local * cache
    score_scale = 1.0 / math.sqrt(head_dim)
    bs = min(16, ps)
    per = ps // bs

    def attend(i):
        @pl.when(lax.rem(i, per) == 0)
        def _():
            for c in cache_copies(i // per):
                c.wait()

        base = pl.multiple_of(i * (bs * pad_heads), bs * pad_heads)
        rows = pl.ds(base, bs * pad_heads)
        qq = q3[rows, :]
        hi = qq.astype(bf16).astype(f32)
        rest = qq - hi
        mid = rest.astype(bf16).astype(f32)
        low = rest - mid
        row_id = lax.broadcasted_iota(jnp.int32, (pad_heads, span), 0)
        col_id = lax.broadcasted_iota(jnp.int32, (pad_heads, span), 1)
        mine = jnp.minimum(row_id // group, kv_local - 1) == col_id // cache
        pos = lax.rem(col_id, cache)
        scored = []
        for b in range(bs):
            sl = slice(b * pad_heads, (b + 1) * pad_heads)
            stack = jnp.concatenate([hi[sl], mid[sl], low[sl]], axis=0).astype(bf16)
            keys = k_b[i * bs + b].reshape(span, head_dim)
            dots = nt_dot(stack, keys)
            sc = (
                dots[:pad_heads]
                + dots[pad_heads : 2 * pad_heads]
                + dots[2 * pad_heads :]
            ) * score_scale
            live = jnp.logical_and(mine, pos < len_b[i * bs + b])
            scored.append(jnp.where(live, sc, -1e30))
        sc = jnp.concatenate(scored, axis=0)
        top = jnp.max(sc, axis=-1, keepdims=True)
        w = jnp.exp(sc - top)
        top3[rows, :] = jnp.broadcast_to(top, (bs * pad_heads, head_dim))
        sum3[rows, :] = jnp.broadcast_to(
            jnp.sum(w, axis=-1, keepdims=True), (bs * pad_heads, head_dim)
        )
        for b in range(bs):
            sl = slice(b * pad_heads, (b + 1) * pad_heads)
            vals = v_b[i * bs + b].reshape(span, head_dim)
            here = pl.ds(base + b * pad_heads, pad_heads)
            c3[here, :] = nn_dot(w[sl].astype(bf16), vals)

    def merge(i):
        rows = pl.ds(i * (bs * pad_heads), bs * pad_heads)
        own = jnp.sum(q3[rows, :] * nk3[rows, :], axis=-1, keepdims=True) * score_scale
        top = jnp.maximum(top3[rows, :], own)
        old = jnp.exp(top3[rows, :] - top)
        new = jnp.exp(own - top)
        scale = 1.0 / (sum3[rows, :] * old + new)
        c3[rows, :] = c3[rows, :] * (old * scale) + (new * scale).astype(bf16).astype(
            f32
        ) * nv3[rows, :]

    tile = min(1024, wide)

    def finish_wave(wave):
        for i in range(wave * ws // bs, (wave + 1) * ws // bs):
            merge(i)
        for h in range(heads):
            ctx[wave * ws : (wave + 1) * ws, h * head_dim : (h + 1) * head_dim] = c3[
                pl.ds(wave * ws * pad_heads + h, ws, stride=pad_heads), :
            ].astype(bf16)

    def hop(d, wave, up):
        rows = pl.ds(pl.multiple_of(wave * ws, ws), ws)
        slot = d + up
        return remote(
            rs_s.at[d, rows], rs_r.at[slot, rows], rs_ssem,
            rs_rsem.at[slot, wave], r, t + 2 * up - 1,
        )

    def pass_on(i, wave):
        d = dest(i)
        up = jnp.where(d > t, 1, 0)
        rows = pl.ds(pl.multiple_of(wave * ws, ws), ws)
        for j in range(wide // tile):
            cols = slice(j * tile, (j + 1) * tile)
            part_f[:, cols] = nn_dot(ctx[rows, :], wo_b[d, :, cols])
        fed = jnp.where(d > t, t > 0, t < n - 1)

        @pl.when(fed)
        def _():
            hop(d, wave, up).wait_recv()
            rs_s[d, rows, :] = (part_f[...] + rs_r[d + up, rows, :].astype(f32)).astype(bf16)

        @pl.when(jnp.logical_not(fed))
        def _():
            rs_s[d, rows, :] = part_f[...].astype(bf16)

        hop(d, wave, up).start()

    waves = rs_rsem.shape[1]
    ws = seqs // waves
    blocks = ws // bs
    ahead = min(2, waves)
    pl.loop(0, blocks)(attend)
    across(1)
    to_planes(2)
    to_planes(3)
    pl.loop(blocks, ahead * blocks)(attend)
    settled(1)
    new_pair()
    at_end = jnp.logical_or(t == 0, t == n - 1)
    for wave in range(waves):
        if wave >= ahead:
            pl.loop(wave * blocks, (wave + 1) * blocks)(attend)
        finish_wave(wave)
        if wave == 0:
            wo_copy(dest(0)).wait()

        @pl.when(at_end)
        def _():
            pass_on(0, wave)

    across(2)
    settled(2)
    down_t = jnp.concatenate([g_od[s] for s in range(reps)], axis=1)
    mid_part = nt_dot(ctx[...], down_t)
    share(packed(mid_part), mid_s, mid_r, mid_ssem, mid_rsem)

    @pl.loop(jnp.where(at_end, 1, 0), n - 1)
    def _(i):
        @pl.when(i > 0)
        def _():
            wo_copy(dest(i)).wait()

        @pl.loop(0, waves)
        def _(wave):
            pass_on(i, wave)

    across(3)
    wo_copy(t).wait()
    for j in range(wide // tile):
        cols = slice(j * tile, (j + 1) * tile)
        own_acc[:, cols] = nn_dot(ctx[...], wo_b[t, :, cols])
    settled(3)
    middle = gather_sum(mid_part, mid_r, mid_rsem)
    up_full = jnp.concatenate([g_ou[s] for s in range(reps)], axis=1)
    own_acc[...] += adapter_scale * nn_dot(middle, up_full)

    @pl.loop(0, waves)
    def _(wave):
        rows = pl.ds(pl.multiple_of(wave * ws, ws), ws)

        @pl.when(t < n - 1)
        def _():
            hop(t, wave, 0).wait_recv()
            own_acc[rows, :] += rs_r[t, rows, :].astype(f32)

        @pl.when(t > 0)
        def _():
            hop(t, wave, 1).wait_recv()
            own_acc[rows, :] += rs_r[t + 1, rows, :].astype(f32)

        out[rows, :] = own_acc[rows, :].astype(bf16)

    for part in range(2):
        whole(dn_b.at[pl.ds(0, reps - 1), ranks[part]], dn_ssem.at[part]).wait()
    for f in range(len(spread)):
        whole(spread[f].at[pl.ds(0, half_reps - 1)], a_ssem.at[f]).wait()
        whole(gathered[f].at[pl.ds(0, groups * (n - 1))], g_ssem.at[f]).wait()
        whole(gathered[f].at[pl.ds(0, groups * n)], g_fsem.at[f]).wait()
    shared(q_part, inner_r.at[0], in_ssem.at[0]).wait()
    shared(kv_part, inner_r.at[1], in_ssem.at[1]).wait()
    shared(mid_part, mid_r, mid_ssem).wait()
    whole(rs_s.at[pl.ds(0, n - 1)], rs_ssem).wait()


def local(
    hidden,
    norm_gain,
    query_weight_matrix,
    key_value_weight,
    output_weight_matrix,
    input_down_factors,
    query_up_factor,
    key_value_up_factors,
    output_down_factor,
    output_up_factor,
    cache_keys,
    cache_values,
    lengths,
):
    reps, n = lax.axis_size("rep"), lax.axis_size("tp")
    r, t = lax.axis_index("rep"), lax.axis_index("tp")
    seqs, depth = hidden.shape
    _, kv_local, cache, head_dim = cache_keys.shape
    width = query_weight_matrix.shape[1]
    heads = width // head_dim
    rank = input_down_factors.shape[2]
    block = input_down_factors.shape[1]
    win = max(block, LANES)

    down = jnp.swapaxes(input_down_factors, 1, 2).reshape(3 * rank, block)
    if win != block:
        spot = lax.rem((r * n + t) * block, win)
        down = lax.dynamic_update_slice(
            jnp.zeros((3 * rank, win), down.dtype), down, (0, spot)
        )
    f_q = query_up_factor
    f_kv = jnp.swapaxes(key_value_up_factors, 1, 2)
    f_od = output_down_factor.T
    f_ou = output_up_factor
    factors = (f_q, f_kv, f_od, f_ou)
    dims = dict(
        tp=n, rep=reps, rank=rank, block=block, win=win,
    )
    pad_heads = -(-heads // 8) * 8
    wide = depth // n
    rows = seqs * pad_heads
    steps, parts, waves = 8, 2, seqs // 16
    dma = pltpu.SemaphoreType.DMA
    hbm = pl.BlockSpec(memory_space=pl.ANY)
    vmem = pl.BlockSpec(memory_space=pltpu.VMEM)
    vec = pltpu.VMEM
    return pl.pallas_call(
        functools.partial(kernel, dims),
        name="decode_block",
        out_shape=pltpu.VMEM((seqs, wide), bf16),
        in_specs=[hbm] * 13,
        out_specs=vmem,
        scratch_shapes=[
            vec((depth,), bf16),
            pltpu.SMEM((seqs,), jnp.int32),
            vec((seqs, depth), bf16),
            vec((seqs, depth), bf16),
            vec((depth, width), bf16),
            vec((2, depth, kv_local * head_dim), bf16),
            vec((n, width, wide), bf16),
            vec((seqs, kv_local, cache, head_dim), bf16),
            vec((seqs, kv_local, cache, head_dim), bf16),
            vec((reps, 3 * rank, win), bf16),
            *[vec((reps // 2,) + f.shape, bf16) for f in factors],
            *[vec((reps,) + f.shape, bf16) for f in factors],
            vec((seqs, head_dim), f32),
            vec((seqs, width), f32),
            vec((2, seqs, kv_local * head_dim), f32),
            vec((2, seqs, 2 * rank), bf16),
            vec((2, n, seqs, 2 * rank), bf16),
            *[vec((rows, head_dim), f32)] * 6,
            vec((seqs, width), bf16),
            vec((seqs, 2 * rank), bf16),
            vec((n, seqs, 2 * rank), bf16),
            vec((seqs // waves, wide), f32),
            vec((seqs, wide), f32),
            vec((n, seqs, wide), bf16),
            vec((n + 1, seqs, wide), bf16),
            dma((2,)),
            dma,
            dma((steps,)),
            dma((steps,)),
            dma((n,)),
            dma((parts,)),
            dma((parts,)),
            dma((1 + len(factors),)),
            dma((2,)),
            dma((2, 2)),
            dma((len(factors),)),
            dma((len(factors),)),
            dma((len(factors),)),
            dma((len(factors), 2)),
            dma((len(factors),)),
            dma((2,)),
            dma((2,)),
            dma,
            dma,
            dma,
            dma((n + 1, waves)),
            pltpu.SemaphoreType.REGULAR((n - 2,)),
        ],
        compiler_params=pltpu.CompilerParams(
            collective_id=0, has_side_effects=True, vmem_limit_bytes=66000000
        ),
    )(
        hidden,
        norm_gain,
        query_weight_matrix,
        key_value_weight,
        output_weight_matrix,
        down,
        *factors,
        cache_keys,
        cache_values,
        lengths,
    )


def solution(mesh):
    return jax.shard_map(
        local,
        mesh=mesh,
        in_specs=(
            P("rep", None),
            P(),
            P(None, "tp"),
            P(None, None, "tp"),
            P("tp", None),
            P(None, ("rep", "tp"), None),
            P(None, ("rep", "tp")),
            P(None, None, ("rep", "tp")),
            P(("rep", "tp"), None),
            P(None, ("rep", "tp")),
            P("rep", "tp", None, None),
            P("rep", "tp", None, None),
            P("rep"),
        ),
        out_specs=P("rep", "tp"),
        check_vma=False,
    )
```

```python
import functools
import math

import jax
import jax.numpy as jnp
from jax import lax
from jax.experimental import pallas as pl
from jax.experimental.pallas import tpu as pltpu
from jax.sharding import PartitionSpec as P

epsilon = 1e-06
rope_base = 1000000.0
adapter_scale = 0.5

f32 = jnp.float32
bf16 = jnp.bfloat16
LANES = 128
MESH_ID = pl.DeviceIdType.MESH


def nt_dot(left, right):
    return lax.dot_general(
        left, right, (((1,), (1,)), ((), ())), preferred_element_type=f32
    )


def nn_dot(left, right):
    return jnp.dot(left, right, preferred_element_type=f32)


def kernel(
    dims,
    hidden,
    gain,
    wq,
    wkv,
    wo,
    dn_own,
    f_q,
    f_kv,
    f_od,
    f_ou,
    cache_k,
    cache_v,
    lengths,
    out,
    gain_b,
    len_b,
    hid_b,
    norm_b,
    wq_b,
    wkv_b,
    wo_b,
    k_b,
    v_b,
    dn_b,
    a_q,
    a_kv,
    a_od,
    a_ou,
    g_q,
    g_kv,
    g_od,
    g_ou,
    angle,
    q_acc,
    kv_acc,
    inner_s,
    inner_r,
    q3,
    nk3,
    nv3,
    c3,
    top3,
    sum3,
    ctx,
    mid_s,
    mid_r,
    part_f,
    own_acc,
    rs_s,
    rs_r,
    small_sem,
    hid_sem,
    w_sem,
    kv_sem,
    wo_sem,
    k_sem,
    v_sem,
    own_sem,
    dn_ssem,
    dn_rsem,
    a_ssem,
    a_rsem,
    g_ssem,
    g_rsem,
    g_fsem,
    in_ssem,
    in_rsem,
    mid_ssem,
    mid_rsem,
    rs_ssem,
    rs_rsem,
    ready,
):
    n, reps = dims["tp"], dims["rep"]
    seqs, depth = hidden.shape
    head_dim = cache_k.shape[3]
    kv_local = cache_k.shape[1]
    heads = wq.shape[1] // head_dim
    group = heads // kv_local
    pad_heads = q3.shape[0] // seqs
    rank = dims["rank"]
    block, win = dims["block"], dims["win"]
    half_reps = reps // 2
    r = lax.axis_index("rep")
    t = lax.axis_index("tp")
    core = lax.rem(r, 2)
    partner = r + 1 - 2 * core

    barrier = pltpu.get_barrier_semaphore()

    def greet(rr, tt):
        pl.semaphore_signal(barrier, inc=1, device_id=(rr, tt), device_id_type=MESH_ID)

    count = 0
    below, above = t > 0, t < n - 1

    @pl.when(below)
    def _():
        greet(r, t - 1)

    @pl.when(above)
    def _():
        greet(r, t + 1)

    beside = jnp.where(below, 1, 0) + jnp.where(above, 1, 0)
    for j in range(1, half_reps):
        greet(lax.rem(r + 2 * j, reps), t)
        greet(lax.rem(partner + 2 * j, reps), t)
        count += 2
    greet(partner, t)
    count += 1

    hid = pltpu.make_async_copy(hidden, hid_b, hid_sem)
    hid.start()
    gain_in = pltpu.make_async_copy(gain, gain_b, small_sem.at[0])
    gain_in.start()
    len_in = pltpu.make_async_copy(lengths, len_b, small_sem.at[1])
    len_in.start()
    own_dn = pltpu.make_async_copy(dn_own, dn_b.at[r], own_sem.at[0])
    mine_at = r // 2
    spread = (a_q, a_kv, a_od, a_ou)
    gathered = (g_q, g_kv, g_od, g_ou)
    own_f = [
        pltpu.make_async_copy(src, dst.at[mine_at], own_sem.at[1 + f])
        for f, (src, dst) in enumerate(zip((f_q, f_kv, f_od, f_ou), spread))
    ]
    own_dn.start()
    for c in own_f:
        c.start()
    steps = w_sem.shape[0]
    kc = depth // steps

    def w_copies(i):
        rows = pl.ds(pl.multiple_of(i * kc, kc), kc)
        return (
            pltpu.make_async_copy(wq.at[rows, :], wq_b.at[rows, :], w_sem.at[i]),
            pltpu.make_async_copy(wkv.at[:, rows, :], wkv_b.at[:, rows, :], kv_sem.at[i]),
        )

    @pl.loop(0, steps)
    def _(i):
        for c in w_copies(i):
            c.start()

    parts = k_sem.shape[0]
    ps = seqs // parts

    def cache_copies(i):
        rows = pl.ds(i * ps, ps)
        return (
            pltpu.make_async_copy(cache_k.at[rows], k_b.at[rows], k_sem.at[i]),
            pltpu.make_async_copy(cache_v.at[rows], v_b.at[rows], v_sem.at[i]),
        )

    wide = wo.shape[1] // n
    most, least = jnp.maximum(n - 1 - t, t), jnp.minimum(n - 1 - t, t)
    toward = jnp.where(n - 1 - t > t, 1, -1)

    def dest(i):
        lead = most - least
        late = jnp.maximum(i - lead, 0)
        away = least - late // 2
        side = jnp.where(late % 2 == 0, -toward, toward)
        return t + jnp.where(i < lead, toward * (most - i), side * away)

    def wo_copy(d):
        cols = pl.ds(pl.multiple_of(d * wide, LANES), wide)
        return pltpu.make_async_copy(wo.at[:, cols], wo_b.at[d], wo_sem.at[d])

    @pl.loop(0, parts)
    def _(i):
        for c in cache_copies(i):
            c.start()

    @pl.loop(0, n - 1)
    def _(i):
        wo_copy(dest(i)).start()

    wo_copy(t).start()

    def remote(src, dst, ssem, rsem, rr, tt):
        return pltpu.make_async_remote_copy(
            src_ref=src,
            dst_ref=dst,
            send_sem=ssem,
            recv_sem=rsem,
            device_id=(rr, tt),
            device_id_type=MESH_ID,
        )

    pl.semaphore_wait(barrier, count + beside)

    def tell(k):
        @pl.when(below)
        def _():
            pl.semaphore_signal(
                ready.at[k], inc=1, device_id=(r, t - 1), device_id_type=MESH_ID
            )

        @pl.when(above)
        def _():
            pl.semaphore_signal(
                ready.at[k], inc=1, device_id=(r, t + 1), device_id_type=MESH_ID
            )

    tell(0)
    ranks = (pl.ds(0, rank), pl.ds(rank, 2 * rank))

    def whole(ref, sem):
        return pltpu.make_async_copy(ref, ref, sem)

    def down(src, part, way, rr):
        here = dn_b.at[src, ranks[part]]
        return remote(here, here, dn_ssem.at[part], dn_rsem.at[part, way], rr, t)

    def chip(j):
        if half_reps != 4:
            return lax.rem(mine_at + j, half_reps)
        aside = mine_at + 1 - 2 * lax.rem(mine_at, 2)
        return (half_reps - 1 - mine_at, aside, half_reps - 1 - aside)[j - 1]

    def send_down(part):
        for j in range(1, half_reps):
            down(r, part, 0, 2 * chip(j) + 1 - core).start()
        down(r, part, 1, partner).start()

    def relay_down(part):
        whole(dn_b.at[pl.ds(0, half_reps - 1), ranks[part]], dn_rsem.at[part, 0]).wait()
        for j in range(1, half_reps):
            down(lax.rem(partner + 2 * j, reps), part, 1, partner).start()

    def share_inner(part):
        whole(dn_b.at[pl.ds(0, half_reps), ranks[part]], dn_rsem.at[part, 1]).wait()
        total = jnp.zeros((seqs, (1 + part) * rank), f32)
        for j in range(reps):
            start = (j * n + t) * block
            cols = pl.ds(pl.multiple_of(start // win * win, LANES), win)
            total = total + nt_dot(norm_b[:, cols], dn_b[j, ranks[part]])
        share(packed(total), inner_s.at[part], inner_r.at[part], in_ssem.at[part], in_rsem.at[part])
        return total

    fold = max(1, LANES // rank)
    few = seqs // fold

    def packed(x):
        if x.shape[1] != rank:
            return x
        return jnp.concatenate([x[f * few : (f + 1) * few] for f in range(fold)], axis=1)

    def unpacked(x):
        return jnp.concatenate([x[:, f * rank : (f + 1) * rank] for f in range(fold)], axis=0)

    def share(x, own, others, ssem, rsem):
        size = x.shape[0]
        own[pl.ds(0, size), :] = x.astype(bf16)
        for j in range(1, n):
            remote(
                own.at[pl.ds(0, size)], others.at[j, pl.ds(0, size)], ssem, rsem,
                r, lax.rem(t + j, n),
            ).start()

    def shared(total, others, sem):
        size = few if total.shape[1] == rank else seqs
        return whole(others.at[pl.ds(0, n - 1), pl.ds(0, size)], sem)

    def gather_sum(total, others, rsem):
        shared(total, others, rsem).wait()
        for j in range(1, n):
            got = others[j] if total.shape[1] != rank else unpacked(others[j, :few])
            total = total + got.astype(f32)
        return total.astype(bf16)

    def to_chips(f):
        here = spread[f].at[mine_at]
        own_f[f].wait()
        for j in range(1, half_reps):
            remote(
                here, here, a_ssem.at[f], a_rsem.at[f], 2 * chip(j) + core, t
            ).start()

    per_plane = reps // n
    groups = per_plane // 2

    def to_planes(f):
        buf, full = spread[f], gathered[f]
        whole(buf.at[pl.ds(0, half_reps - 1)], a_rsem.at[f]).wait()
        for i in range(groups):
            s = n * (2 * i + core) + t
            for j in range(1, n):
                plane = lax.rem(t + j, n)
                src = (plane * per_plane + 2 * i) // 2
                remote(
                    buf.at[src], full.at[s], g_ssem.at[f], g_rsem.at[f, 0], r, plane
                ).start()
            src = (t * per_plane + 2 * i) // 2
            pltpu.make_async_copy(buf.at[src], full.at[s], g_rsem.at[f, 0]).start()

    home = r // per_plane
    group_at = n * lax.rem(r, per_plane)
    rooted = home == t

    def to_root(f):
        full = gathered[f]
        here, there = spread[f].at[mine_at], full.at[group_at + t]
        own_f[f].wait()

        @pl.when(rooted)
        def _():
            pltpu.make_async_copy(here, there, g_rsem.at[f, 0]).start()

        @pl.when(jnp.logical_not(rooted))
        def _():
            remote(here, there, g_ssem.at[f], g_rsem.at[f, 0], r, home).start()

    def from_root(f):
        mine = gathered[f].at[pl.ds(group_at, n)]

        @pl.when(rooted)
        def _():
            whole(mine, g_rsem.at[f, 0]).wait()
            for j in range(1, half_reps):
                remote(
                    mine, mine, a_ssem.at[f], a_rsem.at[f], lax.rem(r + 2 * j, reps), t
                ).start()

    def root_settled(f):
        full = gathered[f]

        @pl.when(rooted)
        def _():
            if groups > 1:
                whole(full.at[pl.ds(0, (groups - 1) * n)], a_rsem.at[f]).wait()

        @pl.when(jnp.logical_not(rooted))
        def _():
            whole(full.at[pl.ds(0, groups * n)], a_rsem.at[f]).wait()

    def root_sent(f):
        @pl.when(rooted)
        def _():
            for _j in range(1, half_reps):
                whole(gathered[f].at[pl.ds(0, n)], a_ssem.at[f]).wait()

        @pl.when(jnp.logical_not(rooted))
        def _():
            whole(gathered[f].at[0], g_ssem.at[f]).wait()

    def across(f):
        full = gathered[f]
        if f < 2:
            whole(full.at[pl.ds(0, groups * n)], g_rsem.at[f, 0]).wait()
        else:
            root_settled(f)
        for i in range(groups):
            here = full.at[pl.ds(n * (2 * i + core), n)]
            remote(here, here, g_fsem.at[f], g_rsem.at[f, 1], partner, t).start()

    def settled(f):
        whole(gathered[f].at[pl.ds(0, groups * n)], g_rsem.at[f, 1]).wait()

    own_dn.wait()
    for part in range(2):
        pl.when(core == 0)(functools.partial(send_down, part))
        to_chips(part)
        pl.when(core == 1)(functools.partial(send_down, part))

    gain_in.wait()
    hid.wait()

    @pl.loop(0, seqs // 16)
    def _(i):
        rows = pl.ds(pl.multiple_of(i * 16, 16), 16)
        x = hid_b[rows, :].astype(f32)
        square = jnp.mean(x * x, axis=-1, keepdims=True)
        norm_b[rows, :] = (
            x * lax.rsqrt(square + epsilon) * gain_b[...].astype(f32).reshape(1, depth)
        ).astype(bf16)

    q_acc[...] = jnp.zeros_like(q_acc)
    kv_acc[...] = jnp.zeros_like(kv_acc)

    def project(i, many):
        for j in range(many):
            for c in w_copies(i + j):
                c.wait()
        rows = pl.ds(pl.multiple_of(i * kc, kc), many * kc)
        x = norm_b[:, rows]
        q_acc[...] += nn_dot(x, wq_b[rows, :])
        for j in range(2):
            kv_acc[j] += nn_dot(x, wkv_b[j, rows, :])

    def heard(k):
        if k < n - 2:
            pl.semaphore_wait(ready.at[k], beside)
        if k < n - 3:
            tell(k + 1)

    project(0, 1)
    heard(0)
    project(1, 2)
    for k in range(1, n - 2):
        heard(k)
    project(3, 1)
    to_planes(0)
    to_root(2)
    to_root(3)
    project(4, 1)
    relay_down(0)
    project(5, 1)
    q_part = share_inner(0)
    project(6, 1)
    to_planes(1)
    relay_down(1)
    project(7, 1)
    len_in.wait()

    half_dim = head_dim // 2
    step = lax.rem(lax.broadcasted_iota(jnp.int32, (1, head_dim), 1), half_dim)
    frequency = jnp.exp(step.astype(f32) * (-2.0 * math.log(rope_base) / head_dim))

    @pl.loop(0, seqs // 8)
    def _(i):
        for b in range(8):
            angle[pl.ds(i * 8 + b, 1), :] = len_b[i * 8 + b].astype(f32) * frequency

    cosv = jnp.cos(angle[...])
    sinv = jnp.sin(angle[...])
    lane = lax.broadcasted_iota(jnp.int32, (seqs, head_dim), 1)
    sinv = jnp.where(lane < half_dim, -sinv, sinv)

    def turn(x):
        return x * cosv + pltpu.roll(x, head_dim // 2, 1) * sinv

    across(0)
    kv_part = share_inner(1)
    settled(0)
    inner_q = gather_sum(q_part, inner_r.at[0], in_rsem.at[0])
    q_up = jnp.concatenate([g_q[s] for s in range(reps)], axis=1)
    q = q_acc[...] + adapter_scale * nn_dot(inner_q, q_up)
    for h in range(pad_heads):
        rows = pl.ds(h, seqs, stride=pad_heads)
        if h < heads:
            q3[rows, :] = turn(q[:, h * head_dim : (h + 1) * head_dim])
        else:
            q3[rows, :] = jnp.zeros((seqs, head_dim), f32)

    def rows_of(j):
        w = g_kv.shape[2]
        return g_kv[:, j].astype(f32).reshape(reps * w, rank).astype(bf16)

    def new_pair():
        inner = gather_sum(kv_part, inner_r.at[1], in_rsem.at[1]).astype(f32)
        inner_k = inner[:, :rank].astype(bf16)
        inner_v = inner[:, rank:].astype(bf16)
        nk = kv_acc[0] + adapter_scale * nt_dot(inner_k, rows_of(0))
        nv = kv_acc[1] + adapter_scale * nt_dot(inner_v, rows_of(1))
        for j in range(kv_local):
            key = turn(nk[:, j * head_dim : (j + 1) * head_dim]).astype(bf16).astype(f32)
            val = nv[:, j * head_dim : (j + 1) * head_dim].astype(bf16).astype(f32)
            for g in range(pad_heads):
                if min(g // group, kv_local - 1) == j:
                    rows = pl.ds(g, seqs, stride=pad_heads)
                    nk3[rows, :] = key
                    nv3[rows, :] = val

    cache = cache_k.shape[2]
    span = kv_local * cache
    score_scale = 1.0 / math.sqrt(head_dim)
    bs = min(16, ps)
    per = ps // bs

    def attend(i):
        @pl.when(lax.rem(i, per) == 0)
        def _():
            for c in cache_copies(i // per):
                c.wait()

        base = pl.multiple_of(i * (bs * pad_heads), bs * pad_heads)
        rows = pl.ds(base, bs * pad_heads)
        qq = q3[rows, :]
        hi = qq.astype(bf16).astype(f32)
        rest = qq - hi
        mid = rest.astype(bf16).astype(f32)
        low = rest - mid
        row_id = lax.broadcasted_iota(jnp.int32, (pad_heads, span), 0)
        col_id = lax.broadcasted_iota(jnp.int32, (pad_heads, span), 1)
        mine = jnp.minimum(row_id // group, kv_local - 1) == col_id // cache
        pos = lax.rem(col_id, cache)
        scored = []
        for b in range(bs):
            sl = slice(b * pad_heads, (b + 1) * pad_heads)
            stack = jnp.concatenate([hi[sl], mid[sl], low[sl]], axis=0).astype(bf16)
            keys = k_b[i * bs + b].reshape(span, head_dim)
            dots = nt_dot(stack, keys)
            sc = (
                dots[:pad_heads]
                + dots[pad_heads : 2 * pad_heads]
                + dots[2 * pad_heads :]
            ) * score_scale
            live = jnp.logical_and(mine, pos < len_b[i * bs + b])
            scored.append(jnp.where(live, sc, -1e30))
        sc = jnp.concatenate(scored, axis=0)
        top = jnp.max(sc, axis=-1, keepdims=True)
        w = jnp.exp(sc - top)
        top3[rows, :] = jnp.broadcast_to(top, (bs * pad_heads, head_dim))
        sum3[rows, :] = jnp.broadcast_to(
            jnp.sum(w, axis=-1, keepdims=True), (bs * pad_heads, head_dim)
        )
        for b in range(bs):
            sl = slice(b * pad_heads, (b + 1) * pad_heads)
            vals = v_b[i * bs + b].reshape(span, head_dim)
            here = pl.ds(base + b * pad_heads, pad_heads)
            c3[here, :] = nn_dot(w[sl].astype(bf16), vals)

    def merge(i):
        rows = pl.ds(i * (bs * pad_heads), bs * pad_heads)
        own = jnp.sum(q3[rows, :] * nk3[rows, :], axis=-1, keepdims=True) * score_scale
        top = jnp.maximum(top3[rows, :], own)
        old = jnp.exp(top3[rows, :] - top)
        new = jnp.exp(own - top)
        scale = 1.0 / (sum3[rows, :] * old + new)
        c3[rows, :] = c3[rows, :] * (old * scale) + (new * scale).astype(bf16).astype(
            f32
        ) * nv3[rows, :]

    tile = min(1024, wide)

    def finish_wave(wave):
        for i in range(wave * ws // bs, (wave + 1) * ws // bs):
            merge(i)
        for h in range(heads):
            ctx[wave * ws : (wave + 1) * ws, h * head_dim : (h + 1) * head_dim] = c3[
                pl.ds(wave * ws * pad_heads + h, ws, stride=pad_heads), :
            ].astype(bf16)

    def hop(d, wave, up, cols=slice(None)):
        rows = pl.ds(pl.multiple_of(wave * ws, ws), ws)
        slot = d + up
        return remote(
            rs_s.at[d, rows, cols], rs_r.at[slot, rows, cols], rs_ssem,
            rs_rsem.at[slot, wave], r, t + 2 * up - 1,
        )

    def pass_on(i, wave):
        d = dest(i)
        up = jnp.where(d > t, 1, 0)
        rows = pl.ds(pl.multiple_of(wave * ws, ws), ws)
        fed = jnp.where(d > t, t > 0, t < n - 1)
        for j in range(wide // tile):
            cols = pl.ds(j * tile, tile)
            part_f[...] = nn_dot(ctx[rows, :], wo_b[d, :, cols])

            @pl.when(fed)
            def _():
                if j == 0:
                    hop(d, wave, up).wait_recv()
                rs_s[d, rows, cols] = (
                    part_f[...] + rs_r[d + up, rows, cols].astype(f32)
                ).astype(bf16)

            @pl.when(jnp.logical_not(fed))
            def _():
                rs_s[d, rows, cols] = part_f[...].astype(bf16)

            hop(d, wave, up, cols).start()

    waves = rs_rsem.shape[1]
    ws = seqs // waves
    blocks = ws // bs
    ahead = min(2, waves)
    pl.loop(0, blocks)(attend)
    across(1)
    from_root(2)
    from_root(3)
    pl.loop(blocks, ahead * blocks)(attend)
    settled(1)
    new_pair()
    at_end = jnp.logical_or(t == 0, t == n - 1)
    for wave in range(waves):
        if wave >= ahead:
            pl.loop(wave * blocks, (wave + 1) * blocks)(attend)
        finish_wave(wave)
        if wave == 0:
            wo_copy(dest(0)).wait()

        @pl.when(at_end)
        def _():
            pass_on(0, wave)

    across(2)
    settled(2)
    down_t = jnp.concatenate([g_od[s] for s in range(reps)], axis=1)
    mid_part = nt_dot(ctx[...], down_t)
    share(packed(mid_part), mid_s, mid_r, mid_ssem, mid_rsem)

    @pl.when(jnp.logical_not(at_end))
    def _():
        @pl.loop(0, waves)
        def _(wave):
            pass_on(0, wave)

    @pl.loop(0, (n - 2) * waves)
    def _(s):
        i = 1 + jnp.where(at_end, s // waves, s % (n - 2))
        wave = jnp.where(at_end, s % waves, s // (n - 2))

        @pl.when(wave == 0)
        def _():
            wo_copy(dest(i)).wait()

        pass_on(i, wave)

    across(3)
    wo_copy(t).wait()
    for j in range(wide // tile):
        cols = slice(j * tile, (j + 1) * tile)
        own_acc[:, cols] = nn_dot(ctx[...], wo_b[t, :, cols])
    settled(3)
    middle = gather_sum(mid_part, mid_r, mid_rsem)
    up_full = jnp.concatenate([g_ou[s] for s in range(reps)], axis=1)
    own_acc[...] += adapter_scale * nn_dot(middle, up_full)

    @pl.loop(0, waves)
    def _(wave):
        rows = pl.ds(pl.multiple_of(wave * ws, ws), ws)

        @pl.when(t < n - 1)
        def _():
            hop(t, wave, 0).wait_recv()
            own_acc[rows, :] += rs_r[t, rows, :].astype(f32)

        @pl.when(t > 0)
        def _():
            hop(t, wave, 1).wait_recv()
            own_acc[rows, :] += rs_r[t + 1, rows, :].astype(f32)

        out[rows, :] = own_acc[rows, :].astype(bf16)

    for part in range(2):
        whole(dn_b.at[pl.ds(0, reps - 1), ranks[part]], dn_ssem.at[part]).wait()
    for f in range(len(spread)):
        if f < 2:
            whole(spread[f].at[pl.ds(0, half_reps - 1)], a_ssem.at[f]).wait()
            whole(gathered[f].at[pl.ds(0, groups * (n - 1))], g_ssem.at[f]).wait()
        else:
            root_sent(f)
        whole(gathered[f].at[pl.ds(0, groups * n)], g_fsem.at[f]).wait()
    shared(q_part, inner_r.at[0], in_ssem.at[0]).wait()
    shared(kv_part, inner_r.at[1], in_ssem.at[1]).wait()
    shared(mid_part, mid_r, mid_ssem).wait()
    whole(rs_s.at[pl.ds(0, n - 1)], rs_ssem).wait()


def local(
    hidden,
    norm_gain,
    query_weight_matrix,
    key_value_weight,
    output_weight_matrix,
    input_down_factors,
    query_up_factor,
    key_value_up_factors,
    output_down_factor,
    output_up_factor,
    cache_keys,
    cache_values,
    lengths,
):
    reps, n = lax.axis_size("rep"), lax.axis_size("tp")
    r, t = lax.axis_index("rep"), lax.axis_index("tp")
    seqs, depth = hidden.shape
    _, kv_local, cache, head_dim = cache_keys.shape
    width = query_weight_matrix.shape[1]
    heads = width // head_dim
    rank = input_down_factors.shape[2]
    block = input_down_factors.shape[1]
    win = max(block, LANES)

    down = jnp.swapaxes(input_down_factors, 1, 2).reshape(3 * rank, block)
    if win != block:
        spot = lax.rem((r * n + t) * block, win)
        down = lax.dynamic_update_slice(
            jnp.zeros((3 * rank, win), down.dtype), down, (0, spot)
        )
    f_q = query_up_factor
    f_kv = jnp.swapaxes(key_value_up_factors, 1, 2)
    f_od = output_down_factor.T
    f_ou = output_up_factor
    factors = (f_q, f_kv, f_od, f_ou)
    dims = dict(
        tp=n, rep=reps, rank=rank, block=block, win=win,
    )
    pad_heads = -(-heads // 8) * 8
    wide = depth // n
    rows = seqs * pad_heads
    steps, parts, waves = 8, 2, seqs // 16
    dma = pltpu.SemaphoreType.DMA
    hbm = pl.BlockSpec(memory_space=pl.ANY)
    vmem = pl.BlockSpec(memory_space=pltpu.VMEM)
    vec = pltpu.VMEM
    return pl.pallas_call(
        functools.partial(kernel, dims),
        name="decode_block",
        out_shape=pltpu.VMEM((seqs, wide), bf16),
        in_specs=[hbm] * 13,
        out_specs=vmem,
        scratch_shapes=[
            vec((depth,), bf16),
            pltpu.SMEM((seqs,), jnp.int32),
            vec((seqs, depth), bf16),
            vec((seqs, depth), bf16),
            vec((depth, width), bf16),
            vec((2, depth, kv_local * head_dim), bf16),
            vec((n, width, wide), bf16),
            vec((seqs, kv_local, cache, head_dim), bf16),
            vec((seqs, kv_local, cache, head_dim), bf16),
            vec((reps, 3 * rank, win), bf16),
            *[vec((reps // 2,) + f.shape, bf16) for f in factors],
            *[vec((reps,) + f.shape, bf16) for f in factors],
            vec((seqs, head_dim), f32),
            vec((seqs, width), f32),
            vec((2, seqs, kv_local * head_dim), f32),
            vec((2, seqs, 2 * rank), bf16),
            vec((2, n, seqs, 2 * rank), bf16),
            *[vec((rows, head_dim), f32)] * 6,
            vec((seqs, width), bf16),
            vec((seqs, 2 * rank), bf16),
            vec((n, seqs, 2 * rank), bf16),
            vec((seqs // waves, min(1024, wide)), f32),
            vec((seqs, wide), f32),
            vec((n, seqs, wide), bf16),
            vec((n + 1, seqs, wide), bf16),
            dma((2,)),
            dma,
            dma((steps,)),
            dma((steps,)),
            dma((n,)),
            dma((parts,)),
            dma((parts,)),
            dma((1 + len(factors),)),
            dma((2,)),
            dma((2, 2)),
            dma((len(factors),)),
            dma((len(factors),)),
            dma((len(factors),)),
            dma((len(factors), 2)),
            dma((len(factors),)),
            dma((2,)),
            dma((2,)),
            dma,
            dma,
            dma,
            dma((n + 1, waves)),
            pltpu.SemaphoreType.REGULAR((n - 2,)),
        ],
        compiler_params=pltpu.CompilerParams(
            collective_id=0, has_side_effects=True, vmem_limit_bytes=66000000
        ),
    )(
        hidden,
        norm_gain,
        query_weight_matrix,
        key_value_weight,
        output_weight_matrix,
        down,
        *factors,
        cache_keys,
        cache_values,
        lengths,
    )


def solution(mesh):
    return jax.shard_map(
        local,
        mesh=mesh,
        in_specs=(
            P("rep", None),
            P(),
            P(None, "tp"),
            P(None, None, "tp"),
            P("tp", None),
            P(None, ("rep", "tp"), None),
            P(None, ("rep", "tp")),
            P(None, None, ("rep", "tp")),
            P(("rep", "tp"), None),
            P(None, ("rep", "tp")),
            P("rep", "tp", None, None),
            P("rep", "tp", None, None),
            P("rep"),
        ),
        out_specs=P("rep", "tp"),
        check_vma=False,
    )
```

```python
import functools
import math

import jax
import jax.numpy as jnp
from jax import lax
from jax.experimental import pallas as pl
from jax.experimental.pallas import tpu as pltpu
from jax.sharding import PartitionSpec as P

epsilon = 1e-06
rope_base = 1000000.0
adapter_scale = 0.5

f32 = jnp.float32
bf16 = jnp.bfloat16
LANES = 128
MESH_ID = pl.DeviceIdType.MESH


def nt_dot(left, right):
    return lax.dot_general(
        left, right, (((1,), (1,)), ((), ())), preferred_element_type=f32
    )


def nn_dot(left, right):
    return jnp.dot(left, right, preferred_element_type=f32)


def kernel(
    dims,
    hidden,
    gain,
    wq,
    wkv,
    wo,
    dn_own,
    f_q,
    f_kv,
    f_od,
    f_ou,
    cache_k,
    cache_v,
    lengths,
    out,
    gain_b,
    len_b,
    hid_b,
    norm_b,
    wq_b,
    wkv_b,
    wo_b,
    k_b,
    v_b,
    dn_b,
    a_q,
    a_kv,
    a_od,
    a_ou,
    g_q,
    g_kv,
    g_od,
    g_ou,
    angle,
    q_acc,
    kv_acc,
    inner_s,
    inner_r,
    q3,
    nk3,
    nv3,
    c3,
    top3,
    sum3,
    ctx,
    mid_s,
    mid_r,
    part_f,
    own_acc,
    rs_s,
    rs_r,
    small_sem,
    hid_sem,
    w_sem,
    kv_sem,
    wo_sem,
    k_sem,
    v_sem,
    own_sem,
    dn_ssem,
    dn_rsem,
    a_ssem,
    a_rsem,
    g_ssem,
    g_rsem,
    g_fsem,
    in_ssem,
    in_rsem,
    mid_ssem,
    mid_rsem,
    rs_ssem,
    rs_rsem,
    ready,
):
    n, reps = dims["tp"], dims["rep"]
    seqs, depth = hidden.shape
    head_dim = cache_k.shape[3]
    kv_local = cache_k.shape[1]
    heads = wq.shape[1] // head_dim
    group = heads // kv_local
    pad_heads = q3.shape[0] // seqs
    rank = dims["rank"]
    block, win = dims["block"], dims["win"]
    half_reps = reps // 2
    r = lax.axis_index("rep")
    t = lax.axis_index("tp")
    core = lax.rem(r, 2)
    partner = r + 1 - 2 * core

    barrier = pltpu.get_barrier_semaphore()

    def greet(rr, tt):
        pl.semaphore_signal(barrier, inc=1, device_id=(rr, tt), device_id_type=MESH_ID)

    count = 0
    below, above = t > 0, t < n - 1

    @pl.when(below)
    def _():
        greet(r, t - 1)

    @pl.when(above)
    def _():
        greet(r, t + 1)

    beside = jnp.where(below, 1, 0) + jnp.where(above, 1, 0)
    for j in range(1, half_reps):
        greet(lax.rem(r + 2 * j, reps), t)
        greet(lax.rem(partner + 2 * j, reps), t)
        count += 2
    greet(partner, t)
    count += 1

    hid = pltpu.make_async_copy(hidden, hid_b, hid_sem)
    hid.start()
    gain_in = pltpu.make_async_copy(gain, gain_b, small_sem.at[0])
    gain_in.start()
    len_in = pltpu.make_async_copy(lengths, len_b, small_sem.at[1])
    len_in.start()
    own_dn = pltpu.make_async_copy(dn_own, dn_b.at[r], own_sem.at[0])
    mine_at = r // 2
    spread = (a_q, a_kv, a_od, a_ou)
    gathered = (g_q, g_kv, g_od, g_ou)
    own_f = [
        pltpu.make_async_copy(src, dst.at[mine_at], own_sem.at[1 + f])
        for f, (src, dst) in enumerate(zip((f_q, f_kv, f_od, f_ou), spread))
    ]
    own_dn.start()
    for c in own_f:
        c.start()
    steps = w_sem.shape[0]
    kc = depth // steps

    def w_copies(i):
        rows = pl.ds(pl.multiple_of(i * kc, kc), kc)
        return (
            pltpu.make_async_copy(wq.at[rows, :], wq_b.at[rows, :], w_sem.at[i]),
            pltpu.make_async_copy(wkv.at[:, rows, :], wkv_b.at[:, rows, :], kv_sem.at[i]),
        )

    @pl.loop(0, steps)
    def _(i):
        for c in w_copies(i):
            c.start()

    parts = k_sem.shape[0]
    ps = seqs // parts

    def cache_copies(i):
        rows = pl.ds(i * ps, ps)
        return (
            pltpu.make_async_copy(cache_k.at[rows], k_b.at[rows], k_sem.at[i]),
            pltpu.make_async_copy(cache_v.at[rows], v_b.at[rows], v_sem.at[i]),
        )

    wide = wo.shape[1] // n
    most, least = jnp.maximum(n - 1 - t, t), jnp.minimum(n - 1 - t, t)
    toward = jnp.where(n - 1 - t > t, 1, -1)

    def dest(i):
        lead = most - least
        late = jnp.maximum(i - lead, 0)
        away = least - late // 2
        side = jnp.where(late % 2 == 0, -toward, toward)
        return t + jnp.where(i < lead, toward * (most - i), side * away)

    def wo_copy(d):
        cols = pl.ds(pl.multiple_of(d * wide, LANES), wide)
        return pltpu.make_async_copy(wo.at[:, cols], wo_b.at[d], wo_sem.at[d])

    @pl.loop(0, parts)
    def _(i):
        for c in cache_copies(i):
            c.start()

    @pl.loop(0, n - 1)
    def _(i):
        wo_copy(dest(i)).start()

    wo_copy(t).start()

    def remote(src, dst, ssem, rsem, rr, tt):
        return pltpu.make_async_remote_copy(
            src_ref=src,
            dst_ref=dst,
            send_sem=ssem,
            recv_sem=rsem,
            device_id=(rr, tt),
            device_id_type=MESH_ID,
        )

    pl.semaphore_wait(barrier, count + beside)

    def tell(k):
        @pl.when(below)
        def _():
            pl.semaphore_signal(
                ready.at[k], inc=1, device_id=(r, t - 1), device_id_type=MESH_ID
            )

        @pl.when(above)
        def _():
            pl.semaphore_signal(
                ready.at[k], inc=1, device_id=(r, t + 1), device_id_type=MESH_ID
            )

    tell(0)
    ranks = (pl.ds(0, rank), pl.ds(rank, 2 * rank))

    def whole(ref, sem):
        return pltpu.make_async_copy(ref, ref, sem)

    def down(src, part, way, rr):
        here = dn_b.at[src, ranks[part]]
        return remote(here, here, dn_ssem.at[part], dn_rsem.at[part, way], rr, t)

    def chip(j):
        if half_reps != 4:
            return lax.rem(mine_at + j, half_reps)
        aside = mine_at + 1 - 2 * lax.rem(mine_at, 2)
        return (half_reps - 1 - mine_at, aside, half_reps - 1 - aside)[j - 1]

    def send_down(part):
        for j in range(1, half_reps):
            down(r, part, 0, 2 * chip(j) + 1 - core).start()
        down(r, part, 1, partner).start()

    def relay_down(part):
        whole(dn_b.at[pl.ds(0, half_reps - 1), ranks[part]], dn_rsem.at[part, 0]).wait()
        for j in range(1, half_reps):
            down(lax.rem(partner + 2 * j, reps), part, 1, partner).start()

    def share_inner(part):
        def some(first):
            total = jnp.zeros((seqs, (1 + part) * rank), f32)
            for k in range(half_reps):
                j = first if k == 0 else lax.rem(r + partner - first + 2 * k, reps)
                start = (j * n + t) * block
                cols = pl.ds(pl.multiple_of(start // win * win, LANES), win)
                total = total + nt_dot(norm_b[:, cols], dn_b[j, ranks[part]])
            return total

        total = some(r)
        whole(dn_b.at[pl.ds(0, half_reps), ranks[part]], dn_rsem.at[part, 1]).wait()
        total = total + some(partner)
        share(packed(total), inner_s.at[part], inner_r.at[part], in_ssem.at[part], in_rsem.at[part])
        return total

    fold = max(1, LANES // rank)
    few = seqs // fold

    def packed(x):
        if x.shape[1] != rank:
            return x
        return jnp.concatenate([x[f * few : (f + 1) * few] for f in range(fold)], axis=1)

    def unpacked(x):
        return jnp.concatenate([x[:, f * rank : (f + 1) * rank] for f in range(fold)], axis=0)

    def share(x, own, others, ssem, rsem):
        size = x.shape[0]
        own[pl.ds(0, size), :] = x.astype(bf16)
        for j in range(1, n):
            remote(
                own.at[pl.ds(0, size)], others.at[j, pl.ds(0, size)], ssem, rsem,
                r, lax.rem(t + j, n),
            ).start()

    def shared(total, others, sem):
        size = few if total.shape[1] == rank else seqs
        return whole(others.at[pl.ds(0, n - 1), pl.ds(0, size)], sem)

    def gather_sum(total, others, rsem):
        shared(total, others, rsem).wait()
        for j in range(1, n):
            got = others[j] if total.shape[1] != rank else unpacked(others[j, :few])
            total = total + got.astype(f32)
        return total.astype(bf16)

    def to_chips(f):
        here = spread[f].at[mine_at]
        own_f[f].wait()
        for j in range(1, half_reps):
            remote(
                here, here, a_ssem.at[f], a_rsem.at[f], 2 * chip(j) + core, t
            ).start()

    per_plane = reps // n
    groups = per_plane // 2

    def to_planes(f):
        buf, full = spread[f], gathered[f]
        whole(buf.at[pl.ds(0, half_reps - 1)], a_rsem.at[f]).wait()
        for i in range(groups):
            s = n * (2 * i + core) + t
            for j in range(1, n):
                plane = lax.rem(t + j, n)
                src = (plane * per_plane + 2 * i) // 2
                remote(
                    buf.at[src], full.at[s], g_ssem.at[f], g_rsem.at[f, 0], r, plane
                ).start()
            src = (t * per_plane + 2 * i) // 2
            pltpu.make_async_copy(buf.at[src], full.at[s], g_rsem.at[f, 0]).start()

    home = r // per_plane
    group_at = n * lax.rem(r, per_plane)
    rooted = home == t

    def to_root(f):
        full = gathered[f]
        here, there = spread[f].at[mine_at], full.at[group_at + t]
        own_f[f].wait()

        @pl.when(rooted)
        def _():
            pltpu.make_async_copy(here, there, g_rsem.at[f, 0]).start()

        @pl.when(jnp.logical_not(rooted))
        def _():
            remote(here, there, g_ssem.at[f], g_rsem.at[f, 0], r, home).start()

    def from_root(f):
        mine = gathered[f].at[pl.ds(group_at, n)]

        @pl.when(rooted)
        def _():
            whole(mine, g_rsem.at[f, 0]).wait()
            for j in range(1, half_reps):
                remote(
                    mine, mine, a_ssem.at[f], a_rsem.at[f], lax.rem(r + 2 * j, reps), t
                ).start()

    def root_settled(f):
        full = gathered[f]

        @pl.when(rooted)
        def _():
            if groups > 1:
                whole(full.at[pl.ds(0, (groups - 1) * n)], a_rsem.at[f]).wait()

        @pl.when(jnp.logical_not(rooted))
        def _():
            whole(full.at[pl.ds(0, groups * n)], a_rsem.at[f]).wait()

    def root_sent(f):
        @pl.when(rooted)
        def _():
            for _j in range(1, half_reps):
                whole(gathered[f].at[pl.ds(0, n)], a_ssem.at[f]).wait()

        @pl.when(jnp.logical_not(rooted))
        def _():
            whole(gathered[f].at[0], g_ssem.at[f]).wait()

    def across(f):
        full = gathered[f]
        if f < 2:
            whole(full.at[pl.ds(0, groups * n)], g_rsem.at[f, 0]).wait()
        else:
            root_settled(f)
        for i in range(groups):
            here = full.at[pl.ds(n * (2 * i + core), n)]
            remote(here, here, g_fsem.at[f], g_rsem.at[f, 1], partner, t).start()

    def settled(f):
        whole(gathered[f].at[pl.ds(0, groups * n)], g_rsem.at[f, 1]).wait()

    own_dn.wait()
    pl.when(core == 0)(functools.partial(send_down, 0))
    to_chips(0)
    pl.when(core == 1)(functools.partial(send_down, 0))
    send_down(1)
    to_chips(1)

    gain_in.wait()
    hid.wait()

    @pl.loop(0, seqs // 16)
    def _(i):
        rows = pl.ds(pl.multiple_of(i * 16, 16), 16)
        x = hid_b[rows, :].astype(f32)
        square = jnp.mean(x * x, axis=-1, keepdims=True)
        norm_b[rows, :] = (
            x * lax.rsqrt(square + epsilon) * gain_b[...].astype(f32).reshape(1, depth)
        ).astype(bf16)

    q_acc[...] = jnp.zeros_like(q_acc)
    kv_acc[...] = jnp.zeros_like(kv_acc)

    def project(i, many):
        for j in range(many):
            for c in w_copies(i + j):
                c.wait()
        rows = pl.ds(pl.multiple_of(i * kc, kc), many * kc)
        x = norm_b[:, rows]
        q_acc[...] += nn_dot(x, wq_b[rows, :])
        for j in range(2):
            kv_acc[j] += nn_dot(x, wkv_b[j, rows, :])

    def heard(k):
        if k < n - 2:
            pl.semaphore_wait(ready.at[k], beside)
        if k < n - 3:
            tell(k + 1)

    project(0, 1)
    heard(0)
    project(1, 2)
    for k in range(1, n - 2):
        heard(k)
    project(3, 1)
    to_planes(0)
    to_root(2)
    to_root(3)
    project(4, 1)
    relay_down(0)
    project(5, 1)
    q_part = share_inner(0)
    project(6, 1)
    to_planes(1)
    relay_down(1)
    project(7, 1)
    len_in.wait()

    half_dim = head_dim // 2
    step = lax.rem(lax.broadcasted_iota(jnp.int32, (1, head_dim), 1), half_dim)
    frequency = jnp.exp(step.astype(f32) * (-2.0 * math.log(rope_base) / head_dim))

    @pl.loop(0, seqs // 8)
    def _(i):
        for b in range(8):
            angle[pl.ds(i * 8 + b, 1), :] = len_b[i * 8 + b].astype(f32) * frequency

    cosv = jnp.cos(angle[...])
    sinv = jnp.sin(angle[...])
    lane = lax.broadcasted_iota(jnp.int32, (seqs, head_dim), 1)
    sinv = jnp.where(lane < half_dim, -sinv, sinv)

    def turn(x):
        return x * cosv + pltpu.roll(x, head_dim // 2, 1) * sinv

    across(0)
    kv_part = share_inner(1)
    settled(0)
    inner_q = gather_sum(q_part, inner_r.at[0], in_rsem.at[0])
    q_up = jnp.concatenate([g_q[s] for s in range(reps)], axis=1)
    q = q_acc[...] + adapter_scale * nn_dot(inner_q, q_up)
    for h in range(pad_heads):
        rows = pl.ds(h, seqs, stride=pad_heads)
        if h < heads:
            q3[rows, :] = turn(q[:, h * head_dim : (h + 1) * head_dim])
        else:
            q3[rows, :] = jnp.zeros((seqs, head_dim), f32)

    def rows_of(j):
        w = g_kv.shape[2]
        return g_kv[:, j].astype(f32).reshape(reps * w, rank).astype(bf16)

    def new_pair():
        inner = gather_sum(kv_part, inner_r.at[1], in_rsem.at[1]).astype(f32)
        inner_k = inner[:, :rank].astype(bf16)
        inner_v = inner[:, rank:].astype(bf16)
        nk = kv_acc[0] + adapter_scale * nt_dot(inner_k, rows_of(0))
        nv = kv_acc[1] + adapter_scale * nt_dot(inner_v, rows_of(1))
        for j in range(kv_local):
            key = turn(nk[:, j * head_dim : (j + 1) * head_dim]).astype(bf16).astype(f32)
            val = nv[:, j * head_dim : (j + 1) * head_dim].astype(bf16).astype(f32)
            for g in range(pad_heads):
                if min(g // group, kv_local - 1) == j:
                    rows = pl.ds(g, seqs, stride=pad_heads)
                    nk3[rows, :] = key
                    nv3[rows, :] = val

    cache = cache_k.shape[2]
    span = kv_local * cache
    score_scale = 1.0 / math.sqrt(head_dim)
    bs = min(16, ps)
    per = ps // bs

    def attend(i):
        @pl.when(lax.rem(i, per) == 0)
        def _():
            for c in cache_copies(i // per):
                c.wait()

        base = pl.multiple_of(i * (bs * pad_heads), bs * pad_heads)
        rows = pl.ds(base, bs * pad_heads)
        qq = q3[rows, :]
        hi = qq.astype(bf16).astype(f32)
        rest = qq - hi
        mid = rest.astype(bf16).astype(f32)
        low = rest - mid
        row_id = lax.broadcasted_iota(jnp.int32, (pad_heads, span), 0)
        col_id = lax.broadcasted_iota(jnp.int32, (pad_heads, span), 1)
        mine = jnp.minimum(row_id // group, kv_local - 1) == col_id // cache
        pos = lax.rem(col_id, cache)
        scored = []
        for b in range(bs):
            sl = slice(b * pad_heads, (b + 1) * pad_heads)
            stack = jnp.concatenate([hi[sl], mid[sl], low[sl]], axis=0).astype(bf16)
            keys = k_b[i * bs + b].reshape(span, head_dim)
            dots = nt_dot(stack, keys)
            sc = (
                dots[:pad_heads]
                + dots[pad_heads : 2 * pad_heads]
                + dots[2 * pad_heads :]
            ) * score_scale
            live = jnp.logical_and(mine, pos < len_b[i * bs + b])
            scored.append(jnp.where(live, sc, -1e30))
        sc = jnp.concatenate(scored, axis=0)
        top = jnp.max(sc, axis=-1, keepdims=True)
        w = jnp.exp(sc - top)
        top3[rows, :] = jnp.broadcast_to(top, (bs * pad_heads, head_dim))
        sum3[rows, :] = jnp.broadcast_to(
            jnp.sum(w, axis=-1, keepdims=True), (bs * pad_heads, head_dim)
        )
        for b in range(bs):
            sl = slice(b * pad_heads, (b + 1) * pad_heads)
            vals = v_b[i * bs + b].reshape(span, head_dim)
            here = pl.ds(base + b * pad_heads, pad_heads)
            c3[here, :] = nn_dot(w[sl].astype(bf16), vals)

    def merge(i):
        rows = pl.ds(i * (bs * pad_heads), bs * pad_heads)
        own = jnp.sum(q3[rows, :] * nk3[rows, :], axis=-1, keepdims=True) * score_scale
        top = jnp.maximum(top3[rows, :], own)
        old = jnp.exp(top3[rows, :] - top)
        new = jnp.exp(own - top)
        scale = 1.0 / (sum3[rows, :] * old + new)
        c3[rows, :] = c3[rows, :] * (old * scale) + (new * scale).astype(bf16).astype(
            f32
        ) * nv3[rows, :]

    tile = min(1024, wide)

    def finish_wave(wave):
        for i in range(wave * ws // bs, (wave + 1) * ws // bs):
            merge(i)
        for h in range(heads):
            ctx[wave * ws : (wave + 1) * ws, h * head_dim : (h + 1) * head_dim] = c3[
                pl.ds(wave * ws * pad_heads + h, ws, stride=pad_heads), :
            ].astype(bf16)

    def hop(d, wave, up, cols=slice(None)):
        rows = pl.ds(pl.multiple_of(wave * ws, ws), ws)
        slot = d + up
        return remote(
            rs_s.at[d, rows, cols], rs_r.at[slot, rows, cols], rs_ssem,
            rs_rsem.at[slot, wave], r, t + 2 * up - 1,
        )

    def pass_on(i, wave):
        d = dest(i)
        up = jnp.where(d > t, 1, 0)
        rows = pl.ds(pl.multiple_of(wave * ws, ws), ws)
        fed = jnp.where(d > t, t > 0, t < n - 1)
        for j in range(wide // tile):
            cols = pl.ds(j * tile, tile)
            part_f[...] = nn_dot(ctx[rows, :], wo_b[d, :, cols])

            @pl.when(fed)
            def _():
                if j == 0:
                    hop(d, wave, up).wait_recv()
                rs_s[d, rows, cols] = (
                    part_f[...] + rs_r[d + up, rows, cols].astype(f32)
                ).astype(bf16)

            @pl.when(jnp.logical_not(fed))
            def _():
                rs_s[d, rows, cols] = part_f[...].astype(bf16)

            hop(d, wave, up, cols).start()

    waves = rs_rsem.shape[1]
    ws = seqs // waves
    blocks = ws // bs
    ahead = min(2, waves)
    pl.loop(0, blocks)(attend)
    across(1)
    from_root(2)
    from_root(3)
    pl.loop(blocks, ahead * blocks)(attend)
    settled(1)
    new_pair()
    at_end = jnp.logical_or(t == 0, t == n - 1)
    for wave in range(waves):
        if wave >= ahead:
            pl.loop(wave * blocks, (wave + 1) * blocks)(attend)
        finish_wave(wave)
        if wave == 0:
            wo_copy(dest(0)).wait()

        @pl.when(at_end)
        def _():
            pass_on(0, wave)

    across(2)
    settled(2)
    down_t = jnp.concatenate([g_od[s] for s in range(reps)], axis=1)
    mid_part = nt_dot(ctx[...], down_t)
    share(packed(mid_part), mid_s, mid_r, mid_ssem, mid_rsem)

    @pl.when(jnp.logical_not(at_end))
    def _():
        @pl.loop(0, waves)
        def _(wave):
            pass_on(0, wave)

    @pl.loop(0, (n - 2) * waves)
    def _(s):
        i = 1 + jnp.where(at_end, s // waves, s % (n - 2))
        wave = jnp.where(at_end, s % waves, s // (n - 2))

        @pl.when(wave == 0)
        def _():
            wo_copy(dest(i)).wait()

        pass_on(i, wave)

    across(3)
    wo_copy(t).wait()
    for j in range(wide // tile):
        cols = slice(j * tile, (j + 1) * tile)
        own_acc[:, cols] = nn_dot(ctx[...], wo_b[t, :, cols])
    settled(3)
    middle = gather_sum(mid_part, mid_r, mid_rsem)
    up_full = jnp.concatenate([g_ou[s] for s in range(reps)], axis=1)
    own_acc[...] += adapter_scale * nn_dot(middle, up_full)

    @pl.loop(0, waves)
    def _(wave):
        rows = pl.ds(pl.multiple_of(wave * ws, ws), ws)

        @pl.when(t < n - 1)
        def _():
            hop(t, wave, 0).wait_recv()
            own_acc[rows, :] += rs_r[t, rows, :].astype(f32)

        @pl.when(t > 0)
        def _():
            hop(t, wave, 1).wait_recv()
            own_acc[rows, :] += rs_r[t + 1, rows, :].astype(f32)

        out[rows, :] = own_acc[rows, :].astype(bf16)

    for part in range(2):
        whole(dn_b.at[pl.ds(0, reps - 1), ranks[part]], dn_ssem.at[part]).wait()
    for f in range(len(spread)):
        if f < 2:
            whole(spread[f].at[pl.ds(0, half_reps - 1)], a_ssem.at[f]).wait()
            whole(gathered[f].at[pl.ds(0, groups * (n - 1))], g_ssem.at[f]).wait()
        else:
            root_sent(f)
        whole(gathered[f].at[pl.ds(0, groups * n)], g_fsem.at[f]).wait()
    shared(q_part, inner_r.at[0], in_ssem.at[0]).wait()
    shared(kv_part, inner_r.at[1], in_ssem.at[1]).wait()
    shared(mid_part, mid_r, mid_ssem).wait()
    whole(rs_s.at[pl.ds(0, n - 1)], rs_ssem).wait()


def local(
    hidden,
    norm_gain,
    query_weight_matrix,
    key_value_weight,
    output_weight_matrix,
    input_down_factors,
    query_up_factor,
    key_value_up_factors,
    output_down_factor,
    output_up_factor,
    cache_keys,
    cache_values,
    lengths,
):
    reps, n = lax.axis_size("rep"), lax.axis_size("tp")
    r, t = lax.axis_index("rep"), lax.axis_index("tp")
    seqs, depth = hidden.shape
    _, kv_local, cache, head_dim = cache_keys.shape
    width = query_weight_matrix.shape[1]
    heads = width // head_dim
    rank = input_down_factors.shape[2]
    block = input_down_factors.shape[1]
    win = max(block, LANES)

    down = jnp.swapaxes(input_down_factors, 1, 2).reshape(3 * rank, block)
    if win != block:
        spot = lax.rem((r * n + t) * block, win)
        down = lax.dynamic_update_slice(
            jnp.zeros((3 * rank, win), down.dtype), down, (0, spot)
        )
    f_q = query_up_factor
    f_kv = jnp.swapaxes(key_value_up_factors, 1, 2)
    f_od = output_down_factor.T
    f_ou = output_up_factor
    factors = (f_q, f_kv, f_od, f_ou)
    dims = dict(
        tp=n, rep=reps, rank=rank, block=block, win=win,
    )
    pad_heads = -(-heads // 8) * 8
    wide = depth // n
    rows = seqs * pad_heads
    steps, parts, waves = 8, 2, seqs // 16
    dma = pltpu.SemaphoreType.DMA
    hbm = pl.BlockSpec(memory_space=pl.ANY)
    vmem = pl.BlockSpec(memory_space=pltpu.VMEM)
    vec = pltpu.VMEM
    return pl.pallas_call(
        functools.partial(kernel, dims),
        name="decode_block",
        out_shape=pltpu.VMEM((seqs, wide), bf16),
        in_specs=[hbm] * 13,
        out_specs=vmem,
        scratch_shapes=[
            vec((depth,), bf16),
            pltpu.SMEM((seqs,), jnp.int32),
            vec((seqs, depth), bf16),
            vec((seqs, depth), bf16),
            vec((depth, width), bf16),
            vec((2, depth, kv_local * head_dim), bf16),
            vec((n, width, wide), bf16),
            vec((seqs, kv_local, cache, head_dim), bf16),
            vec((seqs, kv_local, cache, head_dim), bf16),
            vec((reps, 3 * rank, win), bf16),
            *[vec((reps // 2,) + f.shape, bf16) for f in factors],
            *[vec((reps,) + f.shape, bf16) for f in factors],
            vec((seqs, head_dim), f32),
            vec((seqs, width), f32),
            vec((2, seqs, kv_local * head_dim), f32),
            vec((2, seqs, 2 * rank), bf16),
            vec((2, n, seqs, 2 * rank), bf16),
            *[vec((rows, head_dim), f32)] * 6,
            vec((seqs, width), bf16),
            vec((seqs, 2 * rank), bf16),
            vec((n, seqs, 2 * rank), bf16),
            vec((seqs // waves, min(1024, wide)), f32),
            vec((seqs, wide), f32),
            vec((n, seqs, wide), bf16),
            vec((n + 1, seqs, wide), bf16),
            dma((2,)),
            dma,
            dma((steps,)),
            dma((steps,)),
            dma((n,)),
            dma((parts,)),
            dma((parts,)),
            dma((1 + len(factors),)),
            dma((2,)),
            dma((2, 2)),
            dma((len(factors),)),
            dma((len(factors),)),
            dma((len(factors),)),
            dma((len(factors), 2)),
            dma((len(factors),)),
            dma((2,)),
            dma((2,)),
            dma,
            dma,
            dma,
            dma((n + 1, waves)),
            pltpu.SemaphoreType.REGULAR((n - 2,)),
        ],
        compiler_params=pltpu.CompilerParams(
            collective_id=0, has_side_effects=True, vmem_limit_bytes=66000000
        ),
    )(
        hidden,
        norm_gain,
        query_weight_matrix,
        key_value_weight,
        output_weight_matrix,
        down,
        *factors,
        cache_keys,
        cache_values,
        lengths,
    )


def solution(mesh):
    return jax.shard_map(
        local,
        mesh=mesh,
        in_specs=(
            P("rep", None),
            P(),
            P(None, "tp"),
            P(None, None, "tp"),
            P("tp", None),
            P(None, ("rep", "tp"), None),
            P(None, ("rep", "tp")),
            P(None, None, ("rep", "tp")),
            P(("rep", "tp"), None),
            P(None, ("rep", "tp")),
            P("rep", "tp", None, None),
            P("rep", "tp", None, None),
            P("rep"),
        ),
        out_specs=P("rep", "tp"),
        check_vma=False,
    )
```
